256 devices in a mesh: die: 4 (over x), tile: 64 (over y, z, core).
Axes of the slice: x: 4, y: 4, z: 8, core: 2. Of those that a mesh axis runs over, the one named last changes fastest.
Arguments:
- source_heating: float32 [16, 1024, 2048], P('die', 'tile'), may hold values from -96 to 96, as said below
- material_thermal_values: float32 [6], replicated, may hold values from 0.5 to 8
- layer_material: int32 [16], P('die'), may hold values from 0 to 5
- via_conductance: float32 [4], P('die'), may hold values from 2 to 16
- via_blocks: int32 [4, 24, 4], P('die'), may hold values from 0 to 2048, as said below
Outputs:
- thermal_solution: float32 [16, 1024, 2048], P('die', 'tile')
- balance_defect: float32 [16, 1024, 2048], P('die', 'tile')
The draws below stay inside these ranges and needn't reach their ends.
Inputs may be any that keep to these rules, and one draw needn't show every extreme that they name: `via_blocks`: entry (d, b) is (first row, first column, height, width) of via block b on top of die d, joining die d's top layer to die d + 1's bottom layer, or to the cooled lid for the top die. Height is 8, 16 or 32 and width 16, 32 or 64, each cut to the plane's 1024 x 2048 cells; every block lies inside the plane; blocks may intersect. `source_heating`: heat per cell.
All inputs are finite; a program needn't handle non-finite values.
Results may differ from the reference program's by a relative error of at most 0.0003.
Values sent between devices are 32-bit elements; how exact they have to be, the bound alone decides.
A program may use at most 128 MiB of HBM per device.

```python
import math
import jax
import jax.numpy as jnp
from jax import lax

LZ = 4
NX = 2048
NVIA = 24
NMAT = 6
NU = 2
NC = 6
NDIE = 4
NZ = 16
NY = 1024


def draw_source_heating(key, part):
    key_rough = jax.random.fold_in(key, 0)
    return jnp.clip(16.0 * jax.random.normal(key_rough, (NZ, NY, NX), jnp.float32), -96.0, 96.0)


def draw_via_blocks(key, part):
    keys = jax.random.split(jax.random.fold_in(key, 7), 4)
    tall_pick = jax.random.randint(keys[0], (NDIE, NVIA), 0, 3)
    wide_pick = jax.random.randint(keys[1], (NDIE, NVIA), 0, 3)
    height = jnp.minimum(jnp.array([8, 16, 32], jnp.int32)[tall_pick], NY)
    lateral_extent = jnp.minimum(jnp.array([16, 32, 64], jnp.int32)[wide_pick], NX)
    first_row_index = jax.random.randint(keys[2], (NDIE, NVIA), 0, NY - height + 1)
    col_start = jax.random.randint(keys[3], (NDIE, NVIA), 0, NX - lateral_extent + 1)
    return jnp.stack([first_row_index, col_start, height, lateral_extent], axis=-1).astype(jnp.int32)


def touch_ends(values, key, least, high):
    dims = values.shape
    place = [jax.random.randint(jax.random.fold_in(key, axis), (), 0, dims[axis]) for axis in range(len(dims))]
    values = values.at[tuple(place)].set(least)
    longest = dims.index(max(dims))
    place[longest] = (place[longest] + 1) % dims[longest]
    return values.at[tuple(place)].set(high)


def steps_of(own_key, dims, cuts, smallest, high):
    factor_of = 1.0
    for position, shards_of in cuts:
        draws = jax.random.uniform(jax.random.fold_in(jax.random.fold_in(own_key, 6), position), (shards_of,), jnp.float32, smallest / len(cuts), high / len(cuts))
        factor_of = factor_of * jnp.repeat(jnp.exp(draws), dims[position] // shards_of).reshape((-1,) + (1,) * (len(dims) - 1 - position))
    return factor_of


def setup_inputs(seed: int = 0) -> dict:
    splits = jax.random.split(jax.random.key(seed), 6)
    source_heating = draw_source_heating(jax.random.fold_in(splits[5], 71), 0)
    material_thermal_values = jnp.clip(jnp.exp(jax.random.uniform(splits[1], (NMAT,), jnp.float32, math.log(0.5), math.log(8.0))), 0.5, 8.0)
    layer_material = touch_ends(jax.random.randint(splits[2], (NZ,), 0, NMAT), jax.random.fold_in(splits[2], 1), 0, NMAT - 1).astype(jnp.int32)
    via_conductance = jnp.clip(jnp.exp(math.log(16.0) - 2.0794415 * jax.random.uniform(splits[3], (NDIE,), jnp.float32) ** steps_of(splits[3], (NDIE,), ((0, 4),), -0.2, 0.2)), 2.0, 16.0)
    via_blocks = draw_via_blocks(jax.random.fold_in(splits[5], 71), 0)
    return {"source_heating": source_heating, "material_thermal_values": material_thermal_values, "layer_material": layer_material, "via_conductance": via_conductance, "via_blocks": via_blocks}


OMEGA = 0.8


def block_sums(field):
    depth, height, lateral_extent = field.shape
    return field.reshape(depth, height // 4, 4, lateral_extent // 4, 4).sum(axis=(2, 4))


def spread_out(field):
    return jnp.repeat(jnp.repeat(field, 4, axis=1), 4, axis=2)


def stencil(padded, field, stencil_coefficients, diagonal, upper, lower):
    side = padded[1:-1, 2:, 1:-1] + padded[1:-1, :-2, 1:-1] + padded[1:-1, 1:-1, 2:] + padded[1:-1, 1:-1, :-2]
    return diagonal * field - stencil_coefficients[:, None, None] * side - upper * padded[2:, 1:-1, 1:-1] - lower * padded[:-2, 1:-1, 1:-1]


def reference(source_heating, material_thermal_values, layer_material, via_conductance, via_blocks):
    onehot = (layer_material[:, None] == jnp.arange(NMAT, dtype=jnp.int32)[None, :]).astype(jnp.float32)
    layer_cond = jnp.sum(onehot * material_thermal_values[None, :], axis=1)
    following = jnp.concatenate([layer_cond[1:], layer_cond[-1:]])
    vertical = 2.0 * layer_cond * following / (layer_cond + following)
    row_ids = jnp.arange(NY, dtype=jnp.int32)
    col_ids = jnp.arange(NX, dtype=jnp.int32)

    def die_mask(blocks):
        input_rows = ((row_ids[None, :] >= blocks[:, 0:1]) & (row_ids[None, :] < blocks[:, 0:1] + blocks[:, 2:3])).astype(jnp.float32)
        in_cols = ((col_ids[None, :] >= blocks[:, 1:2]) & (col_ids[None, :] < blocks[:, 1:2] + blocks[:, 3:4])).astype(jnp.float32)
        return jnp.dot(input_rows.T, in_cols, precision=lax.Precision.HIGHEST, preferred_element_type=jnp.float32)

    masks = lax.map(die_mask, via_blocks)
    via_planes = masks * via_conductance[:, None, None]
    via_layers = jnp.repeat(via_planes, LZ, axis=0)
    placed_above = (jnp.arange(NZ, dtype=jnp.int32) % LZ) == LZ - 1
    upper_zero = jnp.where(placed_above[:, None, None], via_layers, vertical[:, None, None])
    lower_zero = jnp.concatenate([jnp.zeros((1, NY, NX), jnp.float32), upper_zero[:-1]], axis=0)
    upper_one = block_sums(upper_zero)
    lower_one = block_sums(lower_zero)
    uppers = [upper_zero, upper_one, block_sums(upper_one)]
    lowers = [lower_zero, lower_one, block_sums(lower_one)]
    stencil_coefficients = [layer_cond, layer_cond * 4.0, layer_cond * 16.0]
    diagonals = [4.0 * stencil_coefficients[lev][:, None, None] + uppers[lev] + lowers[lev] for lev in range(3)]

    def conduction_product(field, level):
        return stencil(jnp.pad(field, 1), field, stencil_coefficients[level], diagonals[level], uppers[level], lowers[level])

    def smooth(field, rhs, level):
        return field + OMEGA * (rhs - conduction_product(field, level)) / diagonals[level]

    def hierarchy_round(level, rhs, field):
        sweeps = NC if level == 2 else NU
        if field is None:
            field = OMEGA * rhs / diagonals[level]
            sweeps = sweeps - 1
        for sweep_index in range(sweeps):
            field = smooth(field, rhs, level)
        if level == 2:
            return field
        remainder = rhs - conduction_product(field, level)
        field = field + spread_out(hierarchy_round(level + 1, block_sums(remainder), None))
        for sweep_index in range(NU):
            field = smooth(field, rhs, level)
        return field

    thermal_solution = hierarchy_round(0, source_heating, None)
    thermal_solution = hierarchy_round(0, source_heating, thermal_solution)
    balance_defect = source_heating - conduction_product(thermal_solution, 0)
    return thermal_solution, balance_defect
```

```python
import functools

import jax
import jax.numpy as jnp
from jax import lax
from jax.experimental import pallas as pl
from jax.experimental.pallas import tpu as pltpu
from jax.sharding import PartitionSpec as P

F32 = jnp.float32
OMEGA = 0.8
KEEP = 1.0 - OMEGA
LZ = 4
ROWS = 16
HY = 6
NYW = ROWS + 2 * HY
NW = 3 * LZ
K = 16
LANES = 128
H1 = 5
N1 = 4 + 2 * H1
H2 = 6
N2 = 1 + 2 * H2
NZ = 16


def rows_of(y, count=1):
    start = y * K
    if not isinstance(start, int):
        start = pl.multiple_of(start, K)
    return pl.ds(start, count * K)


def kernel(n_tile, f_in, pk, v_out, b_out, f, v0, v1, v2, vn, vd_top, wlo, whi, pall, cz,
           turn, restr, r1g, r1, w1, u1, l1, a1, b1, r2, w2, u2, l2, a2, b2, via1, send_sem, recv_sem):
    d = lax.axis_index("die")
    t = lax.axis_index("tile")

    def at(dd, dt):
        return {"die": lax.rem(d + dd + 4, 4), "tile": lax.rem(t + dt + n_tile, n_tile)}

    counter = [0]

    def push(src, dst, dd, dt):
        i = counter[0]
        counter[0] += 1
        copy = pltpu.make_async_remote_copy(
            src_ref=src, dst_ref=dst, send_sem=send_sem.at[i], recv_sem=recv_sem.at[i],
            device_id=at(dd, dt), device_id_type=pl.DeviceIdType.MESH)
        copy.start()
        return copy

    def arrived(copies):
        for copy in copies:
            copy.wait_recv()

    def sent(copies):
        for copy in copies:
            copy.wait_send()

    partners = [(1, 0), (2, 0), (3, 0), (1, 1), (1, -1), (-1, 1), (-1, -1)]
    partners += [(0, s * j) for j in range(1, H2 + 1) for s in (1, -1)]
    barrier = pltpu.get_barrier_semaphore()
    for dd, dt in partners:
        pl.semaphore_signal(barrier, inc=1, device_id=at(dd, dt), device_id_type=pl.DeviceIdType.MESH)

    for m in range(K):
        block = f_in[:, :, m * LANES:(m + 1) * LANES].reshape(LZ * ROWS, LANES)
        turn[m * LANES:(m + 1) * LANES, 0:LZ * ROWS] = block.T
    for k in range(K):
        block = turn[pl.ds(k, LANES, stride=K), 0:LZ * ROWS].T
        for z in range(LZ):
            f[LZ + z, pl.ds(HY * K + k, ROWS, stride=K), :] = block[z * ROWS:(z + 1) * ROWS]
    zero_row = jnp.zeros((K, LANES), F32)

    def clear(y, carry):
        for w in range(NW):
            v2[w, rows_of(y), :] = zero_row
        v1[0, rows_of(y), :] = zero_row
        v1[NW - 1, rows_of(y), :] = zero_row
        return carry

    lax.fori_loop(0, NYW, clear, 0)
    pall[d] = pk[...]

    pl.semaphore_wait(barrier, len(partners))

    own = rows_of(HY, ROWS)
    last = HY + ROWS - 1
    par = [push(pk, pall.at[d], dd, 0) for dd in (1, 2, 3)]
    near = [
        push(f.at[7, own], f.at[3, own], 1, 0),
        push(f.at[4, own], f.at[8, own], -1, 0),
        push(f.at[pl.ds(4, 4), rows_of(last + 1 - HY, HY)], f.at[pl.ds(4, 4), rows_of(0, HY)], 0, 1),
        push(f.at[pl.ds(4, 4), rows_of(HY, HY)], f.at[pl.ds(4, 4), rows_of(HY + ROWS, HY)], 0, -1),
        push(f.at[7, rows_of(last)], f.at[3, rows_of(HY - 1)], 1, 1),
        push(f.at[7, rows_of(HY)], f.at[3, rows_of(last + 1)], 1, -1),
        push(f.at[4, rows_of(last)], f.at[8, rows_of(HY - 1)], -1, 1),
        push(f.at[4, rows_of(HY)], f.at[8, rows_of(last + 1)], -1, -1),
    ]
    bulk = [
        push(f.at[pl.ds(5, 2), own], f.at[pl.ds(1, 2), own], 1, 0),
        push(f.at[pl.ds(5, 2), own], f.at[pl.ds(9, 2), own], -1, 0),
    ]

    arrived(par)

    def coverage(e, rows, row0, cell, lanes_cols):
        n_lanes = lanes_cols * LANES
        prm = pall[e]
        lane = lax.broadcasted_iota(jnp.int32, (24, n_lanes), 1)
        col = (((lane & (LANES - 1)) * lanes_cols + (lane >> 7)) * cell).astype(F32)
        c_lo, c_hi = prm[0:24, 1:2], prm[0:24, 1:2] + prm[0:24, 3:4]
        cols = jnp.maximum(jnp.minimum(c_hi, col + cell) - jnp.maximum(c_lo, col), 0.0)
        row = ((row0 + lax.broadcasted_iota(jnp.int32, (rows, LANES), 0)) * cell).astype(F32)
        r_lo, r_hi = prm[29:30, :], prm[29:30, :] + prm[30:31, :]
        cover = jnp.maximum(jnp.minimum(r_hi, row + cell) - jnp.maximum(r_lo, row), 0.0)
        return jnp.dot(cover[:, 0:24], cols, precision=lax.Precision.HIGHEST,
                       preferred_element_type=F32) * prm[28:29, 0:1]

    cond = jnp.concatenate([pall[e, 24:28, :] for e in range(4)], axis=0)
    follow = jnp.concatenate([cond[1:], cond[NZ - 1:]], axis=0)
    vert = 2.0 * cond * follow / (cond + follow)
    cz[0] = cond
    cz[1] = vert

    zs = lax.broadcasted_iota(jnp.int32, (NZ, LANES), 0)
    is_top = (zs & 3) == 3
    is_end = zs == NZ - 1
    lanes8 = lax.broadcasted_iota(jnp.int32, (8, LANES), 1)
    subs8 = lax.broadcasted_iota(jnp.int32, (8, LANES), 0)
    lanes16 = lax.broadcasted_iota(jnp.int32, (NZ, LANES), 1)

    def valid(row, count):
        return jnp.where((row >= 0) & (row < count), 1.0, 0.0).astype(F32)

    def fine_valid(y):
        return valid(t * ROWS - HY + y, n_tile * ROWS)

    for j in range(4):
        e = lax.rem(d + 2 + j, 4)
        plane = coverage(e, 32, t * ROWS - HY, 1, K)
        for k in range(K):
            vn[j, pl.ds(k, NYW, stride=K), :] = plane[0:NYW, k * LANES:(k + 1) * LANES]

    def zrow(which, w):
        z = lax.rem(LZ * (d + 3) + w, NZ)
        return cz[which, pl.ds(z, 1), :]

    def splat(w):
        ty = w % LZ
        c = zrow(0, w)
        u = zrow(1, w) if ty < 3 else None
        lo = zrow(1, w - 1) if ty > 0 else None
        return c, u, lo

    edge = [jnp.where(lax.rem(d + 2 + j, 4) == 3, 0.0, 1.0).astype(F32) for j in range(4)]
    ends = [(splat(LZ * m), splat(LZ * m + 3)) for m in range(3)]

    def fine_weights(y, carry):
        ok = fine_valid(y) * OMEGA
        planes = [vn[j, rows_of(y), :] for j in range(4)]
        coupled = [planes[j] * edge[j] for j in range(4)]
        vd_top[rows_of(y), :] = planes[2]
        for j in range(4):
            vn[j, rows_of(y), :] = coupled[j]
        for m in range(3):
            (c, u, _), (ct, _, lt) = ends[m]
            wlo[m, rows_of(y), :] = ok / (4.0 * c + u + coupled[m])
            whi[m, rows_of(y), :] = ok / (4.0 * ct + lt + planes[m + 1])
        return carry

    lax.fori_loop(0, NYW, fine_weights, 0)

    def coarse_coeffs(via_rows, scale, couple, row_ok):
        via = jnp.zeros((NZ, LANES), F32)
        for e in range(4):
            via = jnp.where(zs == LZ * e + 3, via_rows[e], via)
        upper = jnp.where(is_top, via, vert * couple)
        nb = jnp.where(is_end, 0.0, upper)
        lower = pltpu.roll(nb, 1, 0)
        return (row_ok * OMEGA) / (4.0 * scale * cond + upper + lower), nb, lower

    for e in range(4):
        plane = coverage(e, 16, t * 4 - H1, 4, 4)
        for p in range(4):
            via1[e, p * 16:(p + 1) * 16, :] = plane[:, p * LANES:(p + 1) * LANES]
        via1[e, 64:80, :] = coverage(e, 16, t - H2, 16, 1)

    def mid_coeffs(i, carry):
        ok = valid(t * 4 - H1 + i, n_tile * 4)
        for p in range(4):
            got = coarse_coeffs([via1[e, pl.ds(p * 16 + i, 1), :] for e in range(4)], 4.0, 16.0, ok)
            w1[i * 4 + p], u1[i * 4 + p], l1[i * 4 + p] = got
        return carry

    lax.fori_loop(0, N1, mid_coeffs, 0)

    def low_coeffs(i, carry):
        ok = valid(t - H2 + i, n_tile)
        got = coarse_coeffs([via1[e, pl.ds(64 + i, 1), :] for e in range(4)], 16.0, 256.0, ok)
        w2[i], u2[i], l2[i] = got
        return carry

    lax.fori_loop(0, N2, low_coeffs, 0)

    def beside(x):
        nxt = pltpu.roll(x, K - 1, 0)
        prv = pltpu.roll(x, 1, 0)
        n_lo, n_hi = nxt[0:8], nxt[8:16]
        p_lo, p_hi = prv[0:8], prv[8:16]
        n_in = jnp.where(lanes8 == LANES - 1, 0.0, pltpu.roll(n_hi, LANES - 1, 1))
        p_in = jnp.where(lanes8 == 0, 0.0, pltpu.roll(p_lo, 1, 1))
        n_hi = jnp.where(subs8 == 7, n_in, n_hi)
        p_lo = jnp.where(subs8 == 0, p_in, p_lo)
        return jnp.concatenate([n_lo + p_lo, n_hi + p_hi], axis=0)

    def flows(src, w, y, consts, above=True, below=True):
        c, u, lo = consts
        ty, m = w % LZ, w // LZ
        x = src[w, rows_of(y), :]
        side = (src[w, rows_of(y - 1), :] + src[w, rows_of(y + 1), :]) + beside(x)
        total = f[w, rows_of(y), :] + c * side
        if above:
            total += (vn[m + 1, rows_of(y), :] if ty == 3 else u) * src[w + 1, rows_of(y), :]
        if below:
            total += (vn[m, rows_of(y), :] if ty == 0 else lo) * src[w - 1, rows_of(y), :]
        return x, total

    def plain_weight(consts):
        c, u, lo = consts
        return OMEGA / (4.0 * c + u + lo)

    def weight(w, y, plain):
        ty, m = w % LZ, w // LZ
        if ty == 0:
            return wlo[m, rows_of(y), :]
        if ty == 3:
            return whi[m, rows_of(y), :]
        return plain * fine_valid(y)

    def layer_consts(layers):
        consts = {w: splat(w) for w in layers}
        plain = {w: plain_weight(consts[w]) for w in layers if w % LZ in (1, 2)}
        return consts, plain

    def start_from_zero(dst, layers, y_lo, y_hi):
        _, plain = layer_consts(layers)

        def body(y, carry):
            for w in layers:
                dst[w, rows_of(y), :] = weight(w, y, plain.get(w)) * f[w, rows_of(y), :]
            return carry

        lax.fori_loop(y_lo, y_hi, body, 0)

    def sweep(src, dst, layers, y_lo, y_hi):
        consts, plain = layer_consts(layers)

        def body(y, carry):
            for w in layers:
                x, total = flows(src, w, y, consts[w])
                dst[w, rows_of(y), :] = KEEP * x + weight(w, y, plain.get(w)) * total
            return carry

        lax.fori_loop(y_lo, y_hi, body, 0)

    def diagonal(w, y, consts):
        c, u, lo = consts
        if w == LZ:
            return 4.0 * c + u + vn[1, rows_of(y), :]
        if w == LZ + 3:
            return 4.0 * c + lo + vd_top[rows_of(y), :]
        return 4.0 * c + u + lo

    own_layers = list(range(LZ, 2 * LZ))

    def restricted_residual(src, slot):
        consts, _ = layer_consts(own_layers)

        def body(i, carry):
            sums = [None] * 6
            for q in range(4):
                y = HY + i * 4 + q
                parts = []
                for w in own_layers:
                    x, total = flows(src, w, y, consts[w], above=w < LZ + 3, below=w > LZ)
                    parts.append(total - diagonal(w, y, consts[w]) * x)
                parts.append(vn[1, rows_of(y), :] * src[LZ, rows_of(y), :])
                parts.append(vn[2, rows_of(y), :] * src[LZ + 3, rows_of(y), :])
                sums = [p if s is None else s + p for s, p in zip(sums, parts)]
            for s in range(6):
                restr[pl.ds(pl.multiple_of((i * 8 + s) * K, K), K), :] = sums[s]
            for s in (6, 7):
                restr[pl.ds(pl.multiple_of((i * 8 + s) * K, K), K), :] = zero_row
            return carry

        lax.fori_loop(0, 4, body, 0)
        for i in range(4):
            for p in range(4):
                tile = restr[pl.ds(i * 128 + 4 * p, 8, stride=K), :]
                for q in range(1, 4):
                    tile += restr[pl.ds(i * 128 + 4 * p + q, 8, stride=K), :]
                r1g[slot, d, i * 4 + p] = tile

    mid_c = 4.0 * cond
    low_c = 16.0 * cond

    def lane_next(x):
        return jnp.where(lanes16 == LANES - 1, 0.0, pltpu.roll(x, LANES - 1, 1))

    def lane_prev(x):
        return jnp.where(lanes16 == 0, 0.0, pltpu.roll(x, 1, 1))

    def mid_flows(src, rhs, i):
        xs = [src[i * 4 + p] for p in range(4)]
        out = []
        for p in range(4):
            nxt = xs[p + 1] if p < 3 else lane_next(xs[0])
            prv = xs[p - 1] if p > 0 else lane_prev(xs[3])
            side = (src[i * 4 - 4 + p] + src[i * 4 + 4 + p]) + (nxt + prv)
            total = rhs[i * 4 + p] + mid_c * side
            total += u1[i * 4 + p] * pltpu.roll(xs[p], NZ - 1, 0)
            total += l1[i * 4 + p] * pltpu.roll(xs[p], 1, 0)
            out.append((xs[p], total))
        return out

    def mid_sweep(src, dst, rhs, lo, hi):
        def body(i, carry):
            for p, (x, total) in enumerate(mid_flows(src, rhs, i)):
                dst[i * 4 + p] = KEEP * x + w1[i * 4 + p] * total
            return carry

        lax.fori_loop(lo, hi, body, 0)

    def assemble(slot):
        def body(i, carry):
            for p in range(4):
                ts = [r1g[slot, e, i * 4 + p] for e in range(4)]

                def put(e, src_row, dst_row):
                    return jnp.where(subs8 == dst_row, pltpu.roll(ts[e], (dst_row - src_row) % 8, 0), 0.0)

                lo = jnp.where(subs8 < 4, ts[0], pltpu.roll(ts[1], 4, 0))
                lo += put(1, 4, 3) + put(0, 5, 4) + put(2, 4, 7)
                hi = jnp.where(subs8 < 4, ts[2], pltpu.roll(ts[3], 4, 0))
                hi += put(1, 5, 0) + put(3, 4, 3) + put(2, 5, 4)
                r1[slot, (H1 + i) * 4 + p] = jnp.concatenate([lo, hi], axis=0)
            return carry

        lax.fori_loop(0, 4, body, 0)

    def coarse_cycle(slot, after_gather, while_waiting):
        gather = [push(r1g.at[slot, d], r1g.at[slot, d], dd, 0) for dd in (1, 3, 2)]
        extra = after_gather()
        arrived(gather)
        assemble(slot)
        rhs = r1.at[slot]
        spread = [
            push(rhs.at[pl.ds(H1 * 4, 16)], rhs.at[pl.ds((H1 - 4) * 4, 16)], 0, 1),
            push(rhs.at[pl.ds(H1 * 4, 16)], rhs.at[pl.ds((H1 + 4) * 4, 16)], 0, -1),
            push(rhs.at[pl.ds((H1 + 3) * 4, 4)], rhs.at[pl.ds(0, 4)], 0, 2),
            push(rhs.at[pl.ds(H1 * 4, 4)], rhs.at[pl.ds((N1 - 1) * 4, 4)], 0, -2),
        ]
        arrived(spread)

        def first(i, carry):
            for p in range(4):
                a1[i * 4 + p] = w1[i * 4 + p] * rhs[i * 4 + p]
            return carry

        lax.fori_loop(0, N1, first, 0)
        mid_sweep(a1, b1, rhs, 1, N1 - 1)

        def down(i, acc):
            for p, (x, total) in enumerate(mid_flows(b1, rhs, i)):
                acc += total - (OMEGA / w1[i * 4 + p]) * x
            return acc

        r2[slot, H2] = lax.fori_loop(H1, H1 + 4, down, jnp.zeros((NZ, LANES), F32))
        low = []
        for j in range(1, H2 + 1):
            low.append(push(r2.at[slot, H2], r2.at[slot, H2 - j], 0, j))
            low.append(push(r2.at[slot, H2], r2.at[slot, H2 + j], 0, -j))
        extra = extra + while_waiting(extra)
        arrived(low)

        bufs = (a2, b2)
        for i in range(N2):
            a2[i] = w2[i] * r2[slot, i]
        for s in range(5):
            src, dst = bufs[s % 2], bufs[(s + 1) % 2]
            for i in range(s + 1, N2 - 1 - s):
                x = src[i]
                side = (src[i - 1] + src[i + 1]) + (lane_next(x) + lane_prev(x))
                total = r2[slot, i] + low_c * side
                total += u2[i] * pltpu.roll(x, NZ - 1, 0) + l2[i] * pltpu.roll(x, 1, 0)
                dst[i] = KEEP * x + w2[i] * total
        fix = bufs[1]
        for g in range(3):
            e2 = fix[H2 - 1 + g]
            for i in range(4):
                for p in range(4):
                    at_cell = (H1 - 4 + g * 4 + i) * 4 + p
                    b1[at_cell] = b1[at_cell] + e2
        mid_sweep(b1, a1, rhs, 2, N1 - 2)
        mid_sweep(a1, b1, rhs, 3, N1 - 3)
        sent(gather + spread + low)
        return extra

    def correction(i, w):
        z = lax.rem(LZ * (d + 3) + w, NZ)
        rows = [b1[i * 4 + p, pl.ds(z, 1), :] for p in range(4)]
        lo = jnp.where(subs8 < 4, rows[0], rows[1])
        hi = jnp.where(subs8 < 4, rows[2], rows[3])
        return jnp.concatenate([lo, hi], axis=0)

    def correct(layers, i_lo, i_hi, edge_rows, pick, dst):
        def row(i, y, fix, w):
            dst[w, rows_of(y), :] = pick(w, y) * fine_valid(y) + fix

        def body(i, carry):
            for w in layers:
                fix = correction(i, w)
                for q in range(4):
                    row(i, HY + (i - H1) * 4 + q, fix, w)
            return carry

        lax.fori_loop(i_lo, i_hi, body, 0)
        for y in edge_rows:
            i = (y - HY) // 4 + H1
            for w in layers:
                row(i, y, correction(i, w), w)

    arrived(near)
    start_from_zero(v0, own_layers, HY - 2, HY + ROWS + 2)
    start_from_zero(v0, [3, 8], HY - 1, HY + ROWS + 1)
    sweep(v0, v1, own_layers, HY - 1, HY + ROWS + 1)
    restricted_residual(v1, 0)

    def background_one():
        return [
            push(f.at[4, own], f.at[0, own], 1, 0),
            push(f.at[7, own], f.at[11, own], -1, 0),
            push(v1.at[4, own], v1.at[0, own], 1, 0),
            push(v1.at[7, own], v1.at[11, own], -1, 0),
            push(v1.at[4, rows_of(last)], v1.at[0, rows_of(HY - 1)], 1, 1),
            push(v1.at[4, rows_of(HY)], v1.at[0, rows_of(last + 1)], 1, -1),
            push(v1.at[7, rows_of(last)], v1.at[11, rows_of(HY - 1)], -1, 1),
            push(v1.at[7, rows_of(HY)], v1.at[11, rows_of(last + 1)], -1, -1),
        ]

    def forward_rows(extra):
        arrived(bulk)
        arrived(extra[0:2])
        hi, lo = last + 1 - HY, HY
        out = []
        for g in (0, 9):
            out.append(push(f.at[pl.ds(g, 3), rows_of(hi, HY)], f.at[pl.ds(g, 3), rows_of(0, HY)], 0, 1))
            out.append(push(f.at[pl.ds(g, 3), rows_of(lo, HY)], f.at[pl.ds(g, 3), rows_of(HY + ROWS, HY)], 0, -1))
        for w in (3, 8):
            out.append(push(f.at[w, rows_of(hi, HY - 1)], f.at[w, rows_of(0, HY - 1)], 0, 1))
            out.append(push(f.at[w, rows_of(lo + 1, HY - 1)], f.at[w, rows_of(HY + ROWS + 1, HY - 1)], 0, -1))
        return out

    extra = coarse_cycle(0, background_one, forward_rows)
    sent(extra[2:8])
    arrived(extra[2:])
    all_layers = list(range(NW))
    inner = list(range(1, NW - 1))
    start_from_zero(v0, all_layers, 0, NYW)
    sweep(v0, v1, inner, 1, NYW - 1)
    correct(all_layers, H1 - 1, H1 + 5, (1, NYW - 2), lambda w, y: v1[w, rows_of(y), :], v1)
    bufs = (v1, v0)
    for s in range(4):
        sweep(bufs[s % 2], bufs[(s + 1) % 2], list(range(s + 1, NW - 1 - s)), s + 2, NYW - 2 - s)
    restricted_residual(v1, 1)

    def background_two():
        return [
            push(v1.at[pl.ds(5, 3), own], v2.at[pl.ds(1, 3), own], 1, 0),
            push(v1.at[pl.ds(4, 3), own], v2.at[pl.ds(8, 3), own], -1, 0),
            push(v1.at[pl.ds(4, 4), rows_of(last - 2, 3)], v2.at[pl.ds(4, 4), rows_of(HY - 3, 3)], 0, 1),
            push(v1.at[pl.ds(4, 4), rows_of(HY, 3)], v2.at[pl.ds(4, 4), rows_of(last + 1, 3)], 0, -1),
            push(v1.at[pl.ds(6, 2), rows_of(last - 1, 2)], v2.at[pl.ds(2, 2), rows_of(HY - 2, 2)], 1, 1),
            push(v1.at[pl.ds(6, 2), rows_of(HY, 2)], v2.at[pl.ds(2, 2), rows_of(last + 1, 2)], 1, -1),
            push(v1.at[pl.ds(4, 2), rows_of(last - 1, 2)], v2.at[pl.ds(8, 2), rows_of(HY - 2, 2)], -1, 1),
            push(v1.at[pl.ds(4, 2), rows_of(HY, 2)], v2.at[pl.ds(8, 2), rows_of(last + 1, 2)], -1, -1),
        ]

    tail = coarse_cycle(1, background_two, lambda extra: [])
    arrived(tail)

    def keep_own(y, carry):
        for w in own_layers:
            v2[w, rows_of(y), :] = v1[w, rows_of(y), :]
        return carry

    lax.fori_loop(HY, HY + ROWS, keep_own, 0)
    deep = list(range(1, NW - 1))
    correct(deep, H1 - 1, H1 + 5, (), lambda w, y: v2[w, rows_of(y), :], v0)
    sent(tail)
    sweep(v0, v1, deep[1:-1], HY - 2, HY + ROWS + 2)
    sweep(v1, v0, deep[2:-2], HY - 1, HY + ROWS + 1)

    consts, _ = layer_consts(own_layers)

    def defect(y, carry):
        for w in own_layers:
            x, total = flows(v0, w, y, consts[w])
            v2[w, rows_of(y), :] = total - diagonal(w, y, consts[w]) * x
        return carry

    lax.fori_loop(HY, HY + ROWS, defect, 0)

    for src, out in ((v0, v_out), (v2, b_out)):
        for k in range(K):
            block = jnp.concatenate([src[w, pl.ds(HY * K + k, ROWS, stride=K), :] for w in own_layers], axis=0)
            turn[pl.ds(k, LANES, stride=K), 0:LZ * ROWS] = block.T
        for m in range(K):
            block = turn[m * LANES:(m + 1) * LANES, 0:LZ * ROWS].T
            out[:, :, m * LANES:(m + 1) * LANES] = block.reshape(LZ, ROWS, LANES)
    sent(par + near + bulk + extra[0:2] + extra[8:])


N_COPIES = 3 + 8 + 2 + 8 + 8 + 8 + 2 * (3 + 4 + 2 * H2)


def local(n_tile, source_heating, material_thermal_values, layer_material, via_conductance, via_blocks):
    onehot = (layer_material[:, None]
              == jnp.arange(material_thermal_values.shape[0], dtype=jnp.int32)[None, :]).astype(F32)
    layer_cond = jnp.sum(onehot * material_thermal_values[None, :], axis=1)
    blocks = via_blocks[0].astype(F32)
    pk = jnp.concatenate([
        jnp.pad(blocks, ((0, 0), (0, LANES - 4))),
        jnp.broadcast_to(layer_cond[:, None], (LZ, LANES)),
        jnp.broadcast_to(via_conductance[:, None], (1, LANES)),
        jnp.pad(blocks.T[0:3:2], ((0, 0), (0, LANES - blocks.shape[0]))),
        jnp.zeros((1, LANES), F32),
    ], axis=0)

    def tiles(*lead):
        return pltpu.VMEM(lead + (NZ, LANES), F32)

    def window(n):
        return pltpu.VMEM((n, NYW * K, LANES), F32)

    vmem = pl.BlockSpec(memory_space=pltpu.VMEM)
    shape = jax.ShapeDtypeStruct(source_heating.shape, F32)
    return pl.pallas_call(
        functools.partial(kernel, n_tile),
        out_shape=(shape, shape),
        in_specs=[vmem, vmem],
        out_specs=(vmem, vmem),
        scratch_shapes=[
            window(NW), window(NW), window(NW), window(NW), window(4),
            pltpu.VMEM((NYW * K, LANES), F32), window(3), window(3),
            pltpu.VMEM((4, 32, LANES), F32), tiles(2),
            pltpu.VMEM((K * LANES, LANES), F32), pltpu.VMEM((4 * 8 * K, LANES), F32),
            pltpu.VMEM((2, 4, 16, 8, LANES), F32), tiles(2, N1 * 4),
            tiles(N1 * 4), tiles(N1 * 4), tiles(N1 * 4), tiles(N1 * 4), tiles(N1 * 4),
            tiles(2, N2), tiles(N2), tiles(N2), tiles(N2), tiles(N2), tiles(N2),
            pltpu.VMEM((4, 80, LANES), F32),
            pltpu.SemaphoreType.DMA((N_COPIES,)),
            pltpu.SemaphoreType.DMA((N_COPIES,)),
        ],
        compiler_params=pltpu.CompilerParams(collective_id=0, has_side_effects=True),
    )(source_heating, pk)


def solution(mesh):
    in_specs = (P("die", "tile", None), P(), P("die"), P("die"), P("die", None, None))
    out_specs = (P("die", "tile", None), P("die", "tile", None))
    body = functools.partial(local, mesh.shape["tile"])
    return jax.shard_map(body, mesh=mesh, in_specs=in_specs, out_specs=out_specs, check_vma=False)
```

```python
import functools

import jax
import jax.numpy as jnp
from jax import lax
from jax.experimental import pallas as pl
from jax.experimental.pallas import tpu as pltpu
from jax.sharding import PartitionSpec as P

F32 = jnp.float32
OMEGA = 0.8
KEEP = 1.0 - OMEGA
LZ = 4
ROWS = 16
HY = 6
NYW = ROWS + 2 * HY
NW = 3 * LZ
K = 16
LANES = 128
H1 = 5
N1 = 4 + 2 * H1
H2 = 6
N2 = 1 + 2 * H2
NZ = 16


def rows_of(y, count=1):
    start = y * K
    if not isinstance(start, int):
        start = pl.multiple_of(start, K)
    return pl.ds(start, count * K)


def row_loop(lo, hi, unroll, fn):
    whole = (hi - lo) // unroll

    def body(i, carry):
        for j in range(unroll):
            fn(lo + i * unroll + j)
        return carry

    if whole:
        lax.fori_loop(0, whole, body, 0)
    for y in range(lo + whole * unroll, hi):
        fn(y)


def kernel(n_tile, f_in, mats, material, via_cond, blocks, v_out, b_out, f, v0, v1, v2, vn, vd_top, wlo, whi, pall, cz,
           turn, restr, r1g, r1, w1, u1, l1, a1, b1, r2, w2, u2, l2, a2, b2, via1, pk, send_sem, recv_sem):
    d = lax.axis_index("die")
    t = lax.axis_index("tile")

    def at(dd, dt):
        return {"die": lax.rem(d + dd + 4, 4), "tile": lax.rem(t + dt + n_tile, n_tile)}

    counter = [0]

    def push(src, dst, dd, dt):
        i = counter[0]
        counter[0] += 1
        copy = pltpu.make_async_remote_copy(
            src_ref=src, dst_ref=dst, send_sem=send_sem.at[i], recv_sem=recv_sem.at[i],
            device_id=at(dd, dt), device_id_type=pl.DeviceIdType.MESH)
        copy.start()
        return copy

    def arrived(copies):
        for copy in copies:
            copy.wait_recv()

    def sent(copies):
        for copy in copies:
            copy.wait_send()

    partners = [(1, 0), (2, 0), (3, 0), (1, 1), (1, -1), (-1, 1), (-1, -1)]
    partners += [(0, s * j) for j in range(1, H2 + 1) for s in (1, -1)]
    barrier = pltpu.get_barrier_semaphore()
    for dd, dt in partners:
        pl.semaphore_signal(barrier, inc=1, device_id=at(dd, dt), device_id_type=pl.DeviceIdType.MESH)

    for m in range(K):
        block = f_in[:, :, m * LANES:(m + 1) * LANES].reshape(LZ * ROWS, LANES)
        turn[m * LANES:(m + 1) * LANES, 0:LZ * ROWS] = block.T
    for k in range(K):
        block = turn[pl.ds(k, LANES, stride=K), 0:LZ * ROWS].T
        for z in range(LZ):
            f[LZ + z, pl.ds(HY * K + k, ROWS, stride=K), :] = block[z * ROWS:(z + 1) * ROWS]
    zero_row = jnp.zeros((K, LANES), F32)

    def clear(y):
        v1[0, rows_of(y), :] = zero_row
        v1[NW - 1, rows_of(y), :] = zero_row

    row_loop(0, NYW, 4, clear)

    pk[0:24, :] = jnp.zeros((24, LANES), F32)
    pk[0:24, 0:4] = blocks[0].astype(F32)
    along = pk[0:24, :].T
    for z in range(LZ):
        pk[24 + z:25 + z, :] = jnp.full((1, LANES), mats[material[z]], F32)
    pk[28:29, :] = jnp.full((1, LANES), via_cond[0], F32)
    pk[29:32, :] = jnp.zeros((3, LANES), F32)
    pk[29:30, 0:24] = along[0:1, :]
    pk[30:31, 0:24] = along[2:3, :]
    pall[d] = pk[...]

    def coverage(e, rows, row0, cell, lanes_cols):
        n_lanes = lanes_cols * LANES
        prm = pall[e]
        lane = lax.broadcasted_iota(jnp.int32, (24, n_lanes), 1)
        col = (((lane & (LANES - 1)) * lanes_cols + (lane >> 7)) * cell).astype(F32)
        c_lo, c_hi = prm[0:24, 1:2], prm[0:24, 1:2] + prm[0:24, 3:4]
        cols = jnp.maximum(jnp.minimum(c_hi, col + cell) - jnp.maximum(c_lo, col), 0.0)
        row = ((row0 + lax.broadcasted_iota(jnp.int32, (rows, LANES), 0)) * cell).astype(F32)
        r_lo, r_hi = prm[29:30, :], prm[29:30, :] + prm[30:31, :]
        cover = jnp.maximum(jnp.minimum(r_hi, row + cell) - jnp.maximum(r_lo, row), 0.0)
        return jnp.dot(cover[:, 0:24], cols, precision=lax.Precision.HIGHEST,
                       preferred_element_type=F32) * prm[28:29, 0:1]

    zs = lax.broadcasted_iota(jnp.int32, (NZ, LANES), 0)
    is_top = (zs & 3) == 3
    is_end = zs == NZ - 1
    lanes8 = lax.broadcasted_iota(jnp.int32, (8, LANES), 1)
    subs8 = lax.broadcasted_iota(jnp.int32, (8, LANES), 0)
    lanes16 = lax.broadcasted_iota(jnp.int32, (NZ, LANES), 1)

    def valid(row, count):
        return jnp.where((row >= 0) & (row < count), 1.0, 0.0).astype(F32)

    def fine_valid(y):
        return valid(t * ROWS - HY + y, n_tile * ROWS)

    def via_plane(j):
        plane = coverage(lax.rem(d + 2 + j, 4), 32, t * ROWS - HY, 1, K)
        for k in range(K):
            vn[j, pl.ds(k, NYW, stride=K), :] = plane[0:NYW, k * LANES:(k + 1) * LANES]

    via_plane(2)
    pl.semaphore_wait(barrier, len(partners))

    own = rows_of(HY, ROWS)
    last = HY + ROWS - 1
    par = [push(pk, pall.at[d], dd, 0) for dd in (1, 2, 3)]
    near = [
        push(f.at[7, own], f.at[3, own], 1, 0),
        push(f.at[4, own], f.at[8, own], -1, 0),
        push(f.at[pl.ds(4, 4), rows_of(last + 1 - HY, HY)], f.at[pl.ds(4, 4), rows_of(0, HY)], 0, 1),
        push(f.at[pl.ds(4, 4), rows_of(HY, HY)], f.at[pl.ds(4, 4), rows_of(HY + ROWS, HY)], 0, -1),
        push(f.at[7, rows_of(last)], f.at[3, rows_of(HY - 1)], 1, 1),
        push(f.at[7, rows_of(HY)], f.at[3, rows_of(last + 1)], 1, -1),
        push(f.at[4, rows_of(last)], f.at[8, rows_of(HY - 1)], -1, 1),
        push(f.at[4, rows_of(HY)], f.at[8, rows_of(last + 1)], -1, -1),
    ]
    bulk = [
        push(f.at[pl.ds(5, 2), own], f.at[pl.ds(1, 2), own], 1, 0),
        push(f.at[pl.ds(5, 2), own], f.at[pl.ds(9, 2), own], -1, 0),
    ]

    def clear_v2(y):
        for w in range(NW):
            v2[w, rows_of(y), :] = zero_row

    row_loop(0, NYW, 2, clear_v2)
    arrived(par)
    via_plane(1)

    cond = jnp.concatenate([pall[e, 24:28, :] for e in range(4)], axis=0)
    follow = jnp.concatenate([cond[1:], cond[NZ - 1:]], axis=0)
    vert = 2.0 * cond * follow / (cond + follow)
    cz[0] = cond
    cz[1] = vert

    def zrow(which, w):
        z = lax.rem(LZ * (d + 3) + w, NZ)
        return cz[which, pl.ds(z, 1), :]

    def splat(w):
        ty = w % LZ
        c = zrow(0, w)
        u = zrow(1, w) if ty < 3 else None
        lo = zrow(1, w - 1) if ty > 0 else None
        return c, u, lo

    edge = [jnp.where(lax.rem(d + 2 + j, 4) == 3, 0.0, 1.0).astype(F32) for j in range(4)]
    ends = [(splat(LZ * m), splat(LZ * m + 3)) for m in range(3)]

    def weight_below(m, y, ok, coupled):
        c, u, _ = ends[m][0]
        wlo[m, rows_of(y), :] = ok / (4.0 * c + u + coupled)

    def weight_above(m, y, ok, plane):
        c, _, lo = ends[m][1]
        whi[m, rows_of(y), :] = ok / (4.0 * c + lo + plane)

    def near_weights(y):
        ok = fine_valid(y) * OMEGA
        planes = {j: vn[j, rows_of(y), :] for j in (1, 2)}
        vd_top[rows_of(y), :] = planes[2]
        for j in (1, 2):
            coupled = planes[j] * edge[j]
            vn[j, rows_of(y), :] = coupled
            weight_below(j, y, ok, coupled)
            weight_above(j - 1, y, ok, planes[j])

    row_loop(0, NYW, 4, near_weights)

    def far_weights(y):
        ok = fine_valid(y) * OMEGA
        planes = {j: vn[j, rows_of(y), :] for j in (0, 3)}
        for j in (0, 3):
            vn[j, rows_of(y), :] = planes[j] * edge[j]
        weight_below(0, y, ok, planes[0] * edge[0])
        weight_above(2, y, ok, planes[3])

    def coarse_coeffs(via_rows, scale, couple, row_ok):
        via = jnp.zeros((NZ, LANES), F32)
        for e in range(4):
            via = jnp.where(zs == LZ * e + 3, via_rows[e], via)
        upper = jnp.where(is_top, via, vert * couple)
        nb = jnp.where(is_end, 0.0, upper)
        lower = pltpu.roll(nb, 1, 0)
        return (row_ok * OMEGA) / (4.0 * scale * cond + upper + lower), nb, lower

    def mid_coeffs(i):
        ok = valid(t * 4 - H1 + i, n_tile * 4)
        for p in range(4):
            got = coarse_coeffs([via1[e, pl.ds(p * 16 + i, 1), :] for e in range(4)], 4.0, 16.0, ok)
            w1[i * 4 + p], u1[i * 4 + p], l1[i * 4 + p] = got

    def low_coeffs(i):
        ok = valid(t - H2 + i, n_tile)
        got = coarse_coeffs([via1[e, pl.ds(64 + i, 1), :] for e in range(4)], 16.0, 256.0, ok)
        w2[i], u2[i], l2[i] = got

    def remaining_coefficients():
        for e in range(4):
            plane = coverage(e, 16, t * 4 - H1, 4, 4)
            for p in range(4):
                via1[e, p * 16:(p + 1) * 16, :] = plane[:, p * LANES:(p + 1) * LANES]
            via1[e, 64:80, :] = coverage(e, 16, t - H2, 16, 1)
        row_loop(0, N1, 2, mid_coeffs)
        row_loop(0, N2, 4, low_coeffs)
        via_plane(0)
        via_plane(3)
        row_loop(0, NYW, 4, far_weights)

    def beside(x):
        nxt = pltpu.roll(x, K - 1, 0)
        prv = pltpu.roll(x, 1, 0)
        n_lo, n_hi = nxt[0:8], nxt[8:16]
        p_lo, p_hi = prv[0:8], prv[8:16]
        n_in = jnp.where(lanes8 == LANES - 1, 0.0, pltpu.roll(n_hi, LANES - 1, 1))
        p_in = jnp.where(lanes8 == 0, 0.0, pltpu.roll(p_lo, 1, 1))
        n_hi = jnp.where(subs8 == 7, n_in, n_hi)
        p_lo = jnp.where(subs8 == 0, p_in, p_lo)
        return jnp.concatenate([n_lo + p_lo, n_hi + p_hi], axis=0)

    def flows(src, w, y, consts, above=True, below=True):
        c, u, lo = consts
        ty, m = w % LZ, w // LZ
        x = src[w, rows_of(y), :]
        side = (src[w, rows_of(y - 1), :] + src[w, rows_of(y + 1), :]) + beside(x)
        total = f[w, rows_of(y), :] + c * side
        if above:
            total += (vn[m + 1, rows_of(y), :] if ty == 3 else u) * src[w + 1, rows_of(y), :]
        if below:
            total += (vn[m, rows_of(y), :] if ty == 0 else lo) * src[w - 1, rows_of(y), :]
        return x, total

    def plain_weight(consts):
        c, u, lo = consts
        return OMEGA / (4.0 * c + u + lo)

    def weight(w, y, plain):
        ty, m = w % LZ, w // LZ
        if ty == 0:
            return wlo[m, rows_of(y), :]
        if ty == 3:
            return whi[m, rows_of(y), :]
        return plain * fine_valid(y)

    def layer_consts(layers):
        consts = {w: splat(w) for w in layers}
        plain = {w: plain_weight(consts[w]) for w in layers if w % LZ in (1, 2)}
        return consts, plain

    def start_from_zero(dst, layers, y_lo, y_hi):
        _, plain = layer_consts(layers)

        def body(y):
            for w in layers:
                dst[w, rows_of(y), :] = weight(w, y, plain.get(w)) * f[w, rows_of(y), :]

        row_loop(y_lo, y_hi, max(1, 16 // len(layers)), body)

    def unroll_of(layers, rows):
        return max(u for u in (1, 2, 3, 4) if rows % u == 0 and u * len(layers) <= 24)

    def sweep(src, dst, layers, y_lo, y_hi):
        consts, plain = layer_consts(layers)

        def body(y):
            for w in layers:
                x, total = flows(src, w, y, consts[w])
                dst[w, rows_of(y), :] = KEEP * x + weight(w, y, plain.get(w)) * total

        row_loop(y_lo, y_hi, unroll_of(layers, y_hi - y_lo), body)

    def diagonal(w, y, consts):
        c, u, lo = consts
        if w == LZ:
            return 4.0 * c + u + vn[1, rows_of(y), :]
        if w == LZ + 3:
            return 4.0 * c + lo + vd_top[rows_of(y), :]
        return 4.0 * c + u + lo

    own_layers = list(range(LZ, 2 * LZ))

    def restricted_residual(src, slot):
        consts, _ = layer_consts(own_layers)

        def body(i, carry):
            sums = [None] * 6
            for q in range(4):
                y = HY + i * 4 + q
                parts = []
                for w in own_layers:
                    x, total = flows(src, w, y, consts[w], above=w < LZ + 3, below=w > LZ)
                    parts.append(total - diagonal(w, y, consts[w]) * x)
                parts.append(vn[1, rows_of(y), :] * src[LZ, rows_of(y), :])
                parts.append(vn[2, rows_of(y), :] * src[LZ + 3, rows_of(y), :])
                sums = [p if s is None else s + p for s, p in zip(sums, parts)]
            for s in range(4):
                restr[pl.ds(pl.multiple_of((i * 4 + s) * K, K), K), :] = sums[s]
            for s in range(2):
                restr[pl.ds(pl.multiple_of(16 * K + (i * 2 + s) * K, K), K), :] = sums[4 + s]
            return carry

        lax.fori_loop(0, 4, body, 0)
        for g, start in enumerate((0, 16 * K, 8 * K)):
            for p in range(4):
                tile = restr[pl.ds(start + 4 * p, 8, stride=K), :]
                for q in range(1, 4):
                    tile += restr[pl.ds(start + 4 * p + q, 8, stride=K), :]
                r1g[slot, d, g * 4 + p] = tile

    mid_c = 4.0 * cond
    low_c = 16.0 * cond

    def lane_next(x):
        return jnp.where(lanes16 == LANES - 1, 0.0, pltpu.roll(x, LANES - 1, 1))

    def lane_prev(x):
        return jnp.where(lanes16 == 0, 0.0, pltpu.roll(x, 1, 1))

    def mid_flows(src, rhs, i):
        xs = [src[i * 4 + p] for p in range(4)]
        out = []
        for p in range(4):
            nxt = xs[p + 1] if p < 3 else lane_next(xs[0])
            prv = xs[p - 1] if p > 0 else lane_prev(xs[3])
            side = (src[i * 4 - 4 + p] + src[i * 4 + 4 + p]) + (nxt + prv)
            total = rhs[i * 4 + p] + mid_c * side
            total += u1[i * 4 + p] * pltpu.roll(xs[p], NZ - 1, 0)
            total += l1[i * 4 + p] * pltpu.roll(xs[p], 1, 0)
            out.append((xs[p], total))
        return out

    def mid_sweep(src, dst, rhs, lo, hi):
        def body(i):
            for p, (x, total) in enumerate(mid_flows(src, rhs, i)):
                dst[i * 4 + p] = KEEP * x + w1[i * 4 + p] * total

        row_loop(lo, hi, 2, body)

    def mid_start(rhs, lo, hi):
        def body(i):
            for p in range(4):
                a1[i * 4 + p] = w1[i * 4 + p] * rhs[i * 4 + p]

        row_loop(lo, hi, 2, body)

    def assemble(slot):
        def turned(x, shift):
            return x if shift % 8 == 0 else pltpu.roll(x, shift % 8, 0)

        for i in range(4):
            half = 4 * (i % 2)
            for p in range(4):
                ts = [r1g[slot, e, (0 if i < 2 else 8) + p] for e in range(4)]
                cs = [r1g[slot, e, 4 + p] for e in range(4)]

                def put(e, down, dst_row):
                    return jnp.where(subs8 == dst_row, turned(cs[e], dst_row - (2 * i + down)), 0.0)

                lo = jnp.where(subs8 < 4, turned(ts[0], -half), turned(ts[1], 4 - half))
                lo += put(1, 0, 3) + put(0, 1, 4) + put(2, 0, 7)
                hi = jnp.where(subs8 < 4, turned(ts[2], -half), turned(ts[3], 4 - half))
                hi += put(1, 1, 0) + put(3, 0, 3) + put(2, 1, 4)
                r1[slot, (H1 + i) * 4 + p] = jnp.concatenate([lo, hi], axis=0)

    def coarse_cycle(slot, after_gather, after_spread, while_waiting):
        gather = [push(r1g.at[slot, d], r1g.at[slot, d], dd, 0) for dd in (2, 1, 3)]
        after_gather()
        arrived(gather)
        assemble(slot)
        rhs = r1.at[slot]

        def mid_rows(i, count):
            return rhs.at[pl.ds(i * 4, count * 4)]

        urgent = [
            push(mid_rows(H1 + 2, 2), mid_rows(H1 - 2, 2), 0, 1),
            push(mid_rows(H1, 2), mid_rows(H1 + 4, 2), 0, -1),
        ]
        rest = [
            push(mid_rows(H1, 2), mid_rows(H1 - 4, 2), 0, 1),
            push(mid_rows(H1 + 2, 2), mid_rows(H1 + 6, 2), 0, -1),
            push(mid_rows(H1 + 3, 1), mid_rows(0, 1), 0, 2),
            push(mid_rows(H1, 1), mid_rows(N1 - 1, 1), 0, -2),
        ]
        after_spread()
        arrived(urgent)
        mid_start(rhs, H1 - 2, H1 + 6)
        mid_sweep(a1, b1, rhs, H1 - 1, H1 + 5)

        def down(i, acc):
            for j in range(2):
                row = H1 + 2 * i + j
                for p, (x, total) in enumerate(mid_flows(b1, rhs, row)):
                    acc += total - (OMEGA / w1[row * 4 + p]) * x
            return acc

        r2[slot, H2] = lax.fori_loop(0, 2, down, jnp.zeros((NZ, LANES), F32))
        low = []
        for j in range(H2, 0, -1):
            low.append(push(r2.at[slot, H2], r2.at[slot, H2 - j], 0, j))
            low.append(push(r2.at[slot, H2], r2.at[slot, H2 + j], 0, -j))
        arrived(rest)
        mid_start(rhs, 0, H1 - 2)
        mid_start(rhs, H1 + 6, N1)
        mid_sweep(a1, b1, rhs, 1, H1 - 1)
        mid_sweep(a1, b1, rhs, H1 + 5, N1 - 1)
        while_waiting()
        arrived(low)

        bufs = (a2, b2)
        for i in range(N2):
            a2[i] = w2[i] * r2[slot, i]
        for s in range(5):
            src, dst = bufs[s % 2], bufs[(s + 1) % 2]
            for i in range(s + 1, N2 - 1 - s):
                x = src[i]
                side = (src[i - 1] + src[i + 1]) + (lane_next(x) + lane_prev(x))
                total = r2[slot, i] + low_c * side
                total += u2[i] * pltpu.roll(x, NZ - 1, 0) + l2[i] * pltpu.roll(x, 1, 0)
                dst[i] = KEEP * x + w2[i] * total
        fix = bufs[1]
        for g in range(3):
            e2 = fix[H2 - 1 + g]
            for i in range(4):
                for p in range(4):
                    at_cell = (H1 - 4 + g * 4 + i) * 4 + p
                    b1[at_cell] = b1[at_cell] + e2
        mid_sweep(b1, a1, rhs, 2, N1 - 2)
        mid_sweep(a1, b1, rhs, 3, N1 - 3)
        sent(gather + urgent + rest + low)

    def correction(i, w):
        z = lax.rem(LZ * (d + 3) + w, NZ)
        rows = [b1[i * 4 + p, pl.ds(z, 1), :] for p in range(4)]
        lo = jnp.where(subs8 < 4, rows[0], rows[1])
        hi = jnp.where(subs8 < 4, rows[2], rows[3])
        return jnp.concatenate([lo, hi], axis=0)

    def correct(layers, i_lo, i_hi, edge_rows, pick, dst):
        def row(i, y, fix, w):
            dst[w, rows_of(y), :] = pick(w, y) * fine_valid(y) + fix

        def body(i):
            for w in layers:
                fix = correction(i, w)
                for q in range(4):
                    row(i, HY + (i - H1) * 4 + q, fix, w)

        row_loop(i_lo, i_hi, 1, body)
        for y in edge_rows:
            i = (y - HY) // 4 + H1
            for w in layers:
                row(i, y, correction(i, w), w)

    arrived(near)
    start_from_zero(v0, own_layers, HY - 2, HY + ROWS + 2)
    start_from_zero(v0, [3, 8], HY - 1, HY + ROWS + 1)
    sweep(v0, v1, own_layers, HY - 1, HY + ROWS + 1)
    restricted_residual(v1, 0)

    later = []
    forwarded = []
    far_source = []
    all_layers = list(range(NW))
    inner = list(range(1, NW - 1))

    def background_one():
        far_source.extend([
            push(f.at[4, own], f.at[0, own], 1, 0),
            push(f.at[7, own], f.at[11, own], -1, 0),
        ])
        later.extend([
            push(v1.at[4, own], v1.at[0, own], 1, 0),
            push(v1.at[7, own], v1.at[11, own], -1, 0),
            push(v1.at[4, rows_of(last)], v1.at[0, rows_of(HY - 1)], 1, 1),
            push(v1.at[4, rows_of(HY)], v1.at[0, rows_of(last + 1)], 1, -1),
            push(v1.at[7, rows_of(last)], v1.at[11, rows_of(HY - 1)], -1, 1),
            push(v1.at[7, rows_of(HY)], v1.at[11, rows_of(last + 1)], -1, -1),
        ])
        remaining_coefficients()

    def forward_rows():
        arrived(bulk + far_source)
        for far in range(1, 5):
            count = HY - far if far > 1 else HY - 2
            low_row, high_row = far, last + 1 + (1 if far == 1 else 0)
            for w in (LZ - far, 2 * LZ - 1 + far):
                forwarded.append(push(f.at[w, rows_of(low_row + ROWS, count)], f.at[w, rows_of(low_row, count)], 0, 1))
                forwarded.append(push(f.at[w, rows_of(high_row - ROWS, count)], f.at[w, rows_of(high_row, count)], 0, -1))

    def presmooth_window():
        arrived(forwarded)
        sent(later)
        start_from_zero(v0, all_layers, 0, NYW)
        sweep(v0, v1, inner, 1, NYW - 1)

    coarse_cycle(0, background_one, forward_rows, presmooth_window)
    arrived(later)
    correct(all_layers, H1 - 1, H1 + 5, (1, NYW - 2), lambda w, y: v1[w, rows_of(y), :], v1)
    bufs = (v1, v0)
    for s in range(4):
        sweep(bufs[s % 2], bufs[(s + 1) % 2], list(range(s + 1, NW - 1 - s)), s + 2, NYW - 2 - s)
    restricted_residual(v1, 1)

    tail = []

    def background_two():
        tail.extend([
            push(v1.at[pl.ds(5, 3), own], v2.at[pl.ds(1, 3), own], 1, 0),
            push(v1.at[pl.ds(4, 3), own], v2.at[pl.ds(8, 3), own], -1, 0),
            push(v1.at[pl.ds(4, 4), rows_of(last - 2, 3)], v2.at[pl.ds(4, 4), rows_of(HY - 3, 3)], 0, 1),
            push(v1.at[pl.ds(4, 4), rows_of(HY, 3)], v2.at[pl.ds(4, 4), rows_of(last + 1, 3)], 0, -1),
            push(v1.at[pl.ds(6, 2), rows_of(last - 1, 2)], v2.at[pl.ds(2, 2), rows_of(HY - 2, 2)], 1, 1),
            push(v1.at[pl.ds(6, 2), rows_of(HY, 2)], v2.at[pl.ds(2, 2), rows_of(last + 1, 2)], 1, -1),
            push(v1.at[pl.ds(4, 2), rows_of(last - 1, 2)], v2.at[pl.ds(8, 2), rows_of(HY - 2, 2)], -1, 1),
            push(v1.at[pl.ds(4, 2), rows_of(HY, 2)], v2.at[pl.ds(8, 2), rows_of(last + 1, 2)], -1, -1),
        ])

    coarse_cycle(1, background_two, lambda: None, lambda: None)
    arrived(tail)

    def keep_own(y):
        for w in own_layers:
            v2[w, rows_of(y), :] = v1[w, rows_of(y), :]

    row_loop(HY, HY + ROWS, 4, keep_own)
    deep = list(range(1, NW - 1))
    correct(deep, H1 - 1, H1 + 5, (), lambda w, y: v2[w, rows_of(y), :], v0)
    sent(tail)
    sweep(v0, v1, deep[1:-1], HY - 2, HY + ROWS + 2)
    sweep(v1, v0, deep[2:-2], HY - 1, HY + ROWS + 1)

    consts, _ = layer_consts(own_layers)

    def defect(y):
        for w in own_layers:
            x, total = flows(v0, w, y, consts[w])
            v2[w, rows_of(y), :] = total - diagonal(w, y, consts[w]) * x

    row_loop(HY, HY + ROWS, 4, defect)

    for src, out in ((v0, v_out), (v2, b_out)):
        for k in range(K):
            block = jnp.concatenate([src[w, pl.ds(HY * K + k, ROWS, stride=K), :] for w in own_layers], axis=0)
            turn[pl.ds(k, LANES, stride=K), 0:LZ * ROWS] = block.T
        for m in range(K):
            block = turn[m * LANES:(m + 1) * LANES, 0:LZ * ROWS].T
            out[:, :, m * LANES:(m + 1) * LANES] = block.reshape(LZ, ROWS, LANES)
    sent(par + near + bulk + far_source + forwarded)


N_COPIES = 3 + 8 + 2 + 8 + 16 + 8 + 2 * (3 + 6 + 2 * H2)


def local(n_tile, source_heating, material_thermal_values, layer_material, via_conductance, via_blocks):
    def tiles(*lead):
        return pltpu.VMEM(lead + (NZ, LANES), F32)

    def window(n):
        return pltpu.VMEM((n, NYW * K, LANES), F32)

    vmem = pl.BlockSpec(memory_space=pltpu.VMEM)
    smem = pl.BlockSpec(memory_space=pltpu.SMEM)
    shape = jax.ShapeDtypeStruct(source_heating.shape, F32)
    return pl.pallas_call(
        functools.partial(kernel, n_tile),
        out_shape=(shape, shape),
        in_specs=[vmem, smem, smem, smem, vmem],
        out_specs=(vmem, vmem),
        scratch_shapes=[
            window(NW), window(NW), window(NW), window(NW), window(4),
            pltpu.VMEM((NYW * K, LANES), F32), window(3), window(3),
            pltpu.VMEM((4, 32, LANES), F32), tiles(2),
            pltpu.VMEM((K * LANES, LANES), F32), pltpu.VMEM((4 * 6 * K, LANES), F32),
            pltpu.VMEM((2, 4, 12, 8, LANES), F32), tiles(2, N1 * 4),
            tiles(N1 * 4), tiles(N1 * 4), tiles(N1 * 4), tiles(N1 * 4), tiles(N1 * 4),
            tiles(2, N2), tiles(N2), tiles(N2), tiles(N2), tiles(N2), tiles(N2),
            pltpu.VMEM((4, 80, LANES), F32), pltpu.VMEM((32, LANES), F32),
            pltpu.SemaphoreType.DMA((N_COPIES,)),
            pltpu.SemaphoreType.DMA((N_COPIES,)),
        ],
        compiler_params=pltpu.CompilerParams(collective_id=0, has_side_effects=True),
    )(source_heating, material_thermal_values, layer_material, via_conductance, via_blocks)


def solution(mesh):
    in_specs = (P("die", "tile", None), P(), P("die"), P("die"), P("die", None, None))
    out_specs = (P("die", "tile", None), P("die", "tile", None))
    body = functools.partial(local, mesh.shape["tile"])
    return jax.shard_map(body, mesh=mesh, in_specs=in_specs, out_specs=out_specs, check_vma=False)
```

```python
import functools

import jax
import jax.numpy as jnp
from jax import lax
from jax.experimental import pallas as pl
from jax.experimental.pallas import tpu as pltpu
from jax.sharding import PartitionSpec as P

F32 = jnp.float32
OMEGA = 0.8
KEEP = 1.0 - OMEGA
LZ = 4
ROWS = 16
HY = 6
NYW = ROWS + 2 * HY
NW = 3 * LZ
K = 16
LANES = 128
H1 = 5
N1 = 4 + 2 * H1
H2 = 6
N2 = 1 + 2 * H2
NZ = 16


def rows_of(y, count=1):
    start = y * K
    if not isinstance(start, int):
        start = pl.multiple_of(start, K)
    return pl.ds(start, count * K)


def row_loop(lo, hi, unroll, fn):
    whole = (hi - lo) // unroll

    def body(i, carry):
        for j in range(unroll):
            fn(lo + i * unroll + j)
        return carry

    if whole:
        lax.fori_loop(0, whole, body, 0)
    for y in range(lo + whole * unroll, hi):
        fn(y)


def kernel(n_tile, f_in, mats, material, via_cond, blocks, out, f_vm, f, v0, v1, v2, vn, vd_top, wlo, whi, pall, cz,
           turn, restr, r1g, r1, w1, u1, l1, a1, b1, r2, w2, u2, l2, a2, b2, via1, pk, send_sem, recv_sem, in_sem):
    d = lax.axis_index("die")
    t = lax.axis_index("tile")

    def at(dd, dt):
        return {"die": lax.rem(d + dd + 4, 4), "tile": lax.rem(t + dt + n_tile, n_tile)}

    counter = [0]

    def push(src, dst, dd, dt):
        i = counter[0]
        counter[0] += 1
        copy = pltpu.make_async_remote_copy(
            src_ref=src, dst_ref=dst, send_sem=send_sem.at[i], recv_sem=recv_sem.at[i],
            device_id=at(dd, dt), device_id_type=pl.DeviceIdType.MESH)
        copy.start()
        return copy

    def arrived(copies):
        for copy in copies:
            copy.wait_recv()

    def sent(copies):
        for copy in copies:
            copy.wait_send()

    loads = []
    for g in range(4):
        part = (slice(None), slice(None), pl.ds(g * 4 * LANES, 4 * LANES))
        loads.append(pltpu.make_async_copy(f_in.at[part], f_vm.at[part], in_sem.at[g]))
        loads[g].start()

    partners = [(1, 0), (2, 0), (3, 0), (1, 1), (1, -1), (-1, 1), (-1, -1)]
    partners += [(0, s * j) for j in range(1, H2 + 1) for s in (1, -1)]
    barrier = pltpu.get_barrier_semaphore()
    for dd, dt in partners:
        pl.semaphore_signal(barrier, inc=1, device_id=at(dd, dt), device_id_type=pl.DeviceIdType.MESH)

    for g in range(4):
        loads[g].wait()
        for m in range(4 * g, 4 * g + 4):
            block = f_vm[:, :, m * LANES:(m + 1) * LANES].reshape(LZ * ROWS, LANES)
            turn[m * LANES:(m + 1) * LANES, 0:LZ * ROWS] = block.T
    for k in range(K):
        block = turn[pl.ds(k, LANES, stride=K), 0:LZ * ROWS].T
        for z in range(LZ):
            f[LZ + z, pl.ds(HY * K + k, ROWS, stride=K), :] = block[z * ROWS:(z + 1) * ROWS]
    zero_row = jnp.zeros((K, LANES), F32)

    def clear(y):
        v1[0, rows_of(y), :] = zero_row
        v1[NW - 1, rows_of(y), :] = zero_row

    row_loop(0, NYW, 4, clear)

    pk[0:4, :] = jnp.full((4, LANES), via_cond[0], F32)
    pk[0:4, 0:24] = blocks[0].astype(F32)
    for z in range(LZ):
        pk[4 + z:5 + z, :] = jnp.full((1, LANES), mats[material[z]], F32)
    pall[d] = pk[...]

    def coverage(e, rows, row0, cell, lanes_cols):
        n_lanes = lanes_cols * LANES
        prm = pall[e]
        down = prm.T
        lane = lax.broadcasted_iota(jnp.int32, (24, n_lanes), 1)
        col = (((lane & (LANES - 1)) * lanes_cols + (lane >> 7)) * cell).astype(F32)
        c_lo, c_hi = down[0:24, 1:2], down[0:24, 1:2] + down[0:24, 3:4]
        cols = jnp.maximum(jnp.minimum(c_hi, col + cell) - jnp.maximum(c_lo, col), 0.0)
        row = ((row0 + lax.broadcasted_iota(jnp.int32, (rows, LANES), 0)) * cell).astype(F32)
        r_lo, r_hi = prm[0:1, :], prm[0:1, :] + prm[2:3, :]
        cover = jnp.maximum(jnp.minimum(r_hi, row + cell) - jnp.maximum(r_lo, row), 0.0)
        return jnp.dot(cover[:, 0:24], cols, precision=lax.Precision.HIGHEST,
                       preferred_element_type=F32) * prm[0:1, LANES - 1:]

    zs = lax.broadcasted_iota(jnp.int32, (NZ, LANES), 0)
    is_top = (zs & 3) == 3
    is_end = zs == NZ - 1
    lanes8 = lax.broadcasted_iota(jnp.int32, (8, LANES), 1)
    subs8 = lax.broadcasted_iota(jnp.int32, (8, LANES), 0)
    lanes16 = lax.broadcasted_iota(jnp.int32, (NZ, LANES), 1)

    def valid(row, count):
        return jnp.where((row >= 0) & (row < count), 1.0, 0.0).astype(F32)

    def fine_valid(y):
        return valid(t * ROWS - HY + y, n_tile * ROWS)

    def via_plane(j):
        plane = coverage(lax.rem(d + 2 + j, 4), 32, t * ROWS - HY, 1, K)
        for k in range(K):
            vn[j, pl.ds(k, NYW, stride=K), :] = plane[0:NYW, k * LANES:(k + 1) * LANES]

    via_plane(2)
    pl.semaphore_wait(barrier, len(partners))

    own = rows_of(HY, ROWS)
    last = HY + ROWS - 1
    par = [push(pk, pall.at[d], dd, 0) for dd in (1, 2, 3)]
    near = [
        push(f.at[7, own], f.at[3, own], 1, 0),
        push(f.at[4, own], f.at[8, own], -1, 0),
        push(f.at[pl.ds(4, 4), rows_of(last + 1 - HY, HY)], f.at[pl.ds(4, 4), rows_of(0, HY)], 0, 1),
        push(f.at[pl.ds(4, 4), rows_of(HY, HY)], f.at[pl.ds(4, 4), rows_of(HY + ROWS, HY)], 0, -1),
        push(f.at[7, rows_of(last)], f.at[3, rows_of(HY - 1)], 1, 1),
        push(f.at[7, rows_of(HY)], f.at[3, rows_of(last + 1)], 1, -1),
        push(f.at[4, rows_of(last)], f.at[8, rows_of(HY - 1)], -1, 1),
        push(f.at[4, rows_of(HY)], f.at[8, rows_of(last + 1)], -1, -1),
    ]
    bulk = [
        push(f.at[pl.ds(5, 2), own], f.at[pl.ds(1, 2), own], 1, 0),
        push(f.at[pl.ds(5, 2), own], f.at[pl.ds(9, 2), own], -1, 0),
    ]

    def clear_v2(y):
        for w in range(NW):
            v2[w, rows_of(y), :] = zero_row

    row_loop(0, NYW, 2, clear_v2)
    arrived(par)
    via_plane(1)

    cond = jnp.concatenate([pall[e, 4:8, :] for e in range(4)], axis=0)
    follow = jnp.concatenate([cond[1:], cond[NZ - 1:]], axis=0)
    vert = 2.0 * cond * follow / (cond + follow)
    cz[0] = cond
    cz[1] = vert

    def zrow(which, w):
        z = lax.rem(LZ * (d + 3) + w, NZ)
        return cz[which, pl.ds(z, 1), :]

    def splat(w):
        ty = w % LZ
        c = zrow(0, w)
        u = zrow(1, w) if ty < 3 else None
        lo = zrow(1, w - 1) if ty > 0 else None
        return c, u, lo

    edge = [jnp.where(lax.rem(d + 2 + j, 4) == 3, 0.0, 1.0).astype(F32) for j in range(4)]
    ends = [(splat(LZ * m), splat(LZ * m + 3)) for m in range(3)]

    def weight_below(m, y, ok, coupled):
        c, u, _ = ends[m][0]
        wlo[m, rows_of(y), :] = ok / (4.0 * c + u + coupled)

    def weight_above(m, y, ok, plane):
        c, _, lo = ends[m][1]
        whi[m, rows_of(y), :] = ok / (4.0 * c + lo + plane)

    def near_weights(y):
        ok = fine_valid(y) * OMEGA
        planes = {j: vn[j, rows_of(y), :] for j in (1, 2)}
        vd_top[rows_of(y), :] = planes[2]
        for j in (1, 2):
            coupled = planes[j] * edge[j]
            vn[j, rows_of(y), :] = coupled
            weight_below(j, y, ok, coupled)
            weight_above(j - 1, y, ok, planes[j])

    row_loop(0, NYW, 4, near_weights)

    def far_weights(y):
        ok = fine_valid(y) * OMEGA
        planes = {j: vn[j, rows_of(y), :] for j in (0, 3)}
        for j in (0, 3):
            vn[j, rows_of(y), :] = planes[j] * edge[j]
        weight_below(0, y, ok, planes[0] * edge[0])
        weight_above(2, y, ok, planes[3])

    def coarse_coeffs(via_rows, scale, couple, row_ok):
        via = jnp.zeros((NZ, LANES), F32)
        for e in range(4):
            via = jnp.where(zs == LZ * e + 3, via_rows[e], via)
        upper = jnp.where(is_top, via, vert * couple)
        nb = jnp.where(is_end, 0.0, upper)
        lower = pltpu.roll(nb, 1, 0)
        return (row_ok * OMEGA) / (4.0 * scale * cond + upper + lower), nb, lower

    def mid_coeffs(i):
        ok = valid(t * 4 - H1 + i, n_tile * 4)
        for p in range(4):
            got = coarse_coeffs([via1[e, pl.ds(p * 16 + i, 1), :] for e in range(4)], 4.0, 16.0, ok)
            w1[i * 4 + p], u1[i * 4 + p], l1[i * 4 + p] = got

    def low_coeffs(i):
        ok = valid(t - H2 + i, n_tile)
        got = coarse_coeffs([via1[e, pl.ds(64 + i, 1), :] for e in range(4)], 16.0, 256.0, ok)
        w2[i], u2[i], l2[i] = got

    def remaining_coefficients():
        for e in range(4):
            plane = coverage(e, 16, t * 4 - H1, 4, 4)
            for p in range(4):
                via1[e, p * 16:(p + 1) * 16, :] = plane[:, p * LANES:(p + 1) * LANES]
            via1[e, 64:80, :] = coverage(e, 16, t - H2, 16, 1)
        row_loop(0, N1, 2, mid_coeffs)
        row_loop(0, N2, 4, low_coeffs)
        via_plane(0)
        via_plane(3)
        row_loop(0, NYW, 4, far_weights)

    def beside(x):
        nxt = pltpu.roll(x, K - 1, 0)
        prv = pltpu.roll(x, 1, 0)
        n_lo, n_hi = nxt[0:8], nxt[8:16]
        p_lo, p_hi = prv[0:8], prv[8:16]
        n_in = jnp.where(lanes8 == LANES - 1, 0.0, pltpu.roll(n_hi, LANES - 1, 1))
        p_in = jnp.where(lanes8 == 0, 0.0, pltpu.roll(p_lo, 1, 1))
        n_hi = jnp.where(subs8 == 7, n_in, n_hi)
        p_lo = jnp.where(subs8 == 0, p_in, p_lo)
        return jnp.concatenate([n_lo + p_lo, n_hi + p_hi], axis=0)

    def flows(src, w, y, consts, above=True, below=True):
        c, u, lo = consts
        ty, m = w % LZ, w // LZ
        x = src[w, rows_of(y), :]
        side = (src[w, rows_of(y - 1), :] + src[w, rows_of(y + 1), :]) + beside(x)
        total = f[w, rows_of(y), :] + c * side
        if above:
            total += (vn[m + 1, rows_of(y), :] if ty == 3 else u) * src[w + 1, rows_of(y), :]
        if below:
            total += (vn[m, rows_of(y), :] if ty == 0 else lo) * src[w - 1, rows_of(y), :]
        return x, total

    def plain_weight(consts):
        c, u, lo = consts
        return OMEGA / (4.0 * c + u + lo)

    def weight(w, y, plain):
        ty, m = w % LZ, w // LZ
        if ty == 0:
            return wlo[m, rows_of(y), :]
        if ty == 3:
            return whi[m, rows_of(y), :]
        return plain * fine_valid(y)

    def layer_consts(layers):
        consts = {w: splat(w) for w in layers}
        plain = {w: plain_weight(consts[w]) for w in layers if w % LZ in (1, 2)}
        return consts, plain

    def start_from_zero(dst, layers, y_lo, y_hi):
        _, plain = layer_consts(layers)

        def body(y):
            for w in layers:
                dst[w, rows_of(y), :] = weight(w, y, plain.get(w)) * f[w, rows_of(y), :]

        row_loop(y_lo, y_hi, max(1, 16 // len(layers)), body)

    def unroll_of(layers, rows):
        return max(u for u in (1, 2, 3, 4, 6) if rows % u == 0 and u * len(layers) <= 24)

    def sweep(src, dst, layers, y_lo, y_hi):
        consts, plain = layer_consts(layers)

        def body(y):
            for w in layers:
                x, total = flows(src, w, y, consts[w])
                dst[w, rows_of(y), :] = KEEP * x + weight(w, y, plain.get(w)) * total

        row_loop(y_lo, y_hi, unroll_of(layers, y_hi - y_lo), body)

    def diagonal(w, y, consts):
        c, u, lo = consts
        if w == LZ:
            return 4.0 * c + u + vn[1, rows_of(y), :]
        if w == LZ + 3:
            return 4.0 * c + lo + vd_top[rows_of(y), :]
        return 4.0 * c + u + lo

    own_layers = list(range(LZ, 2 * LZ))

    def restricted_residual(src, slot):
        consts, _ = layer_consts(own_layers)

        def body(i, carry):
            sums = [None] * 6
            for q in range(4):
                y = HY + i * 4 + q
                parts = []
                for w in own_layers:
                    x, total = flows(src, w, y, consts[w], above=w < LZ + 3, below=w > LZ)
                    parts.append(total - diagonal(w, y, consts[w]) * x)
                parts.append(vn[1, rows_of(y), :] * src[LZ, rows_of(y), :])
                parts.append(vn[2, rows_of(y), :] * src[LZ + 3, rows_of(y), :])
                sums = [p if s is None else s + p for s, p in zip(sums, parts)]
            for s in range(4):
                restr[pl.ds(pl.multiple_of((i * 4 + s) * K, K), K), :] = sums[s]
            for s in range(2):
                restr[pl.ds(pl.multiple_of(16 * K + (i * 2 + s) * K, K), K), :] = sums[4 + s]
            return carry

        lax.fori_loop(0, 4, body, 0)
        for g, start in enumerate((0, 16 * K, 8 * K)):
            for p in range(4):
                tile = restr[pl.ds(start + 4 * p, 8, stride=K), :]
                for q in range(1, 4):
                    tile += restr[pl.ds(start + 4 * p + q, 8, stride=K), :]
                r1g[slot, d, g * 4 + p] = tile

    mid_c = 4.0 * cond
    low_c = 16.0 * cond

    def lane_next(x):
        return jnp.where(lanes16 == LANES - 1, 0.0, pltpu.roll(x, LANES - 1, 1))

    def lane_prev(x):
        return jnp.where(lanes16 == 0, 0.0, pltpu.roll(x, 1, 1))

    def mid_flows(src, rhs, i):
        xs = [src[i * 4 + p] for p in range(4)]
        out = []
        for p in range(4):
            nxt = xs[p + 1] if p < 3 else lane_next(xs[0])
            prv = xs[p - 1] if p > 0 else lane_prev(xs[3])
            side = (src[i * 4 - 4 + p] + src[i * 4 + 4 + p]) + (nxt + prv)
            total = rhs[i * 4 + p] + mid_c * side
            total += u1[i * 4 + p] * pltpu.roll(xs[p], NZ - 1, 0)
            total += l1[i * 4 + p] * pltpu.roll(xs[p], 1, 0)
            out.append((xs[p], total))
        return out

    def mid_sweep(src, dst, rhs, lo, hi):
        def body(i):
            for p, (x, total) in enumerate(mid_flows(src, rhs, i)):
                dst[i * 4 + p] = KEEP * x + w1[i * 4 + p] * total

        row_loop(lo, hi, max(u for u in (1, 2, 3, 4, 5) if (hi - lo) % u == 0), body)

    def mid_start(rhs, lo, hi):
        def body(i):
            for p in range(4):
                a1[i * 4 + p] = w1[i * 4 + p] * rhs[i * 4 + p]

        row_loop(lo, hi, 2, body)

    def assemble(slot):
        def turned(x, shift):
            return x if shift % 8 == 0 else pltpu.roll(x, shift % 8, 0)

        for i in range(4):
            half = 4 * (i % 2)
            for p in range(4):
                ts = [r1g[slot, e, (0 if i < 2 else 8) + p] for e in range(4)]
                cs = [r1g[slot, e, 4 + p] for e in range(4)]

                def put(e, down, dst_row):
                    return jnp.where(subs8 == dst_row, turned(cs[e], dst_row - (2 * i + down)), 0.0)

                lo = jnp.where(subs8 < 4, turned(ts[0], -half), turned(ts[1], 4 - half))
                lo += put(1, 0, 3) + put(0, 1, 4) + put(2, 0, 7)
                hi = jnp.where(subs8 < 4, turned(ts[2], -half), turned(ts[3], 4 - half))
                hi += put(1, 1, 0) + put(3, 0, 3) + put(2, 1, 4)
                r1[slot, (H1 + i) * 4 + p] = jnp.concatenate([lo, hi], axis=0)

    def coarse_cycle(slot, after_gather, after_spread, while_waiting):
        gather = [push(r1g.at[slot, d], r1g.at[slot, d], dd, 0) for dd in (2, 1, 3)]
        after_gather()
        arrived(gather)
        assemble(slot)
        rhs = r1.at[slot]

        def mid_rows(i, count):
            return rhs.at[pl.ds(i * 4, count * 4)]

        urgent = [
            push(mid_rows(H1 + 2, 2), mid_rows(H1 - 2, 2), 0, 1),
            push(mid_rows(H1, 2), mid_rows(H1 + 4, 2), 0, -1),
        ]
        rest = [
            push(mid_rows(H1, 2), mid_rows(H1 - 4, 2), 0, 1),
            push(mid_rows(H1 + 2, 2), mid_rows(H1 + 6, 2), 0, -1),
            push(mid_rows(H1 + 3, 1), mid_rows(0, 1), 0, 2),
            push(mid_rows(H1, 1), mid_rows(N1 - 1, 1), 0, -2),
        ]
        after_spread()
        arrived(urgent)
        mid_start(rhs, H1 - 2, H1 + 6)
        mid_sweep(a1, b1, rhs, H1 - 1, H1 + 5)

        def down(i, acc):
            for j in range(2):
                row = H1 + 2 * i + j
                for p, (x, total) in enumerate(mid_flows(b1, rhs, row)):
                    acc += total - (OMEGA / w1[row * 4 + p]) * x
            return acc

        r2[slot, H2] = lax.fori_loop(0, 2, down, jnp.zeros((NZ, LANES), F32))
        low = []
        for j in range(H2, 0, -1):
            low.append(push(r2.at[slot, H2], r2.at[slot, H2 - j], 0, j))
            low.append(push(r2.at[slot, H2], r2.at[slot, H2 + j], 0, -j))
        arrived(rest)
        mid_start(rhs, 0, H1 - 2)
        mid_start(rhs, H1 + 6, N1)
        mid_sweep(a1, b1, rhs, 1, H1 - 1)
        mid_sweep(a1, b1, rhs, H1 + 5, N1 - 1)
        while_waiting()
        arrived(low)

        bufs = (a2, b2)
        for i in range(N2):
            a2[i] = w2[i] * r2[slot, i]
        for s in range(5):
            src, dst = bufs[s % 2], bufs[(s + 1) % 2]
            for i in range(s + 1, N2 - 1 - s):
                x = src[i]
                side = (src[i - 1] + src[i + 1]) + (lane_next(x) + lane_prev(x))
                total = r2[slot, i] + low_c * side
                total += u2[i] * pltpu.roll(x, NZ - 1, 0) + l2[i] * pltpu.roll(x, 1, 0)
                dst[i] = KEEP * x + w2[i] * total
        fix = bufs[1]
        for g in range(3):
            e2 = fix[H2 - 1 + g]
            for i in range(4):
                for p in range(4):
                    at_cell = (H1 - 4 + g * 4 + i) * 4 + p
                    b1[at_cell] = b1[at_cell] + e2
        mid_sweep(b1, a1, rhs, 2, N1 - 2)
        mid_sweep(a1, b1, rhs, 3, N1 - 3)
        sent(gather + urgent + rest + low)

    def correction(i, w):
        z = lax.rem(LZ * (d + 3) + w, NZ)
        rows = [b1[i * 4 + p, pl.ds(z, 1), :] for p in range(4)]
        lo = jnp.where(subs8 < 4, rows[0], rows[1])
        hi = jnp.where(subs8 < 4, rows[2], rows[3])
        return jnp.concatenate([lo, hi], axis=0)

    def correct(layers, i_lo, i_hi, edge_rows, pick, dst):
        def row(i, y, fix, w):
            dst[w, rows_of(y), :] = pick(w, y) * fine_valid(y) + fix

        def body(i):
            for w in layers:
                fix = correction(i, w)
                for q in range(4):
                    row(i, HY + (i - H1) * 4 + q, fix, w)

        row_loop(i_lo, i_hi, 1, body)
        for y in edge_rows:
            i = (y - HY) // 4 + H1
            for w in layers:
                row(i, y, correction(i, w), w)

    arrived(near)
    start_from_zero(v0, own_layers, HY - 2, HY + ROWS + 2)
    start_from_zero(v0, [3, 8], HY - 1, HY + ROWS + 1)
    sweep(v0, v1, own_layers, HY - 1, HY + ROWS + 1)
    restricted_residual(v1, 0)

    later = []
    forwarded = []
    far_source = []
    all_layers = list(range(NW))
    inner = list(range(1, NW - 1))

    def background_one():
        far_source.extend([
            push(f.at[4, own], f.at[0, own], 1, 0),
            push(f.at[7, own], f.at[11, own], -1, 0),
        ])
        later.extend([
            push(v1.at[4, own], v1.at[0, own], 1, 0),
            push(v1.at[7, own], v1.at[11, own], -1, 0),
            push(v1.at[4, rows_of(last)], v1.at[0, rows_of(HY - 1)], 1, 1),
            push(v1.at[4, rows_of(HY)], v1.at[0, rows_of(last + 1)], 1, -1),
            push(v1.at[7, rows_of(last)], v1.at[11, rows_of(HY - 1)], -1, 1),
            push(v1.at[7, rows_of(HY)], v1.at[11, rows_of(last + 1)], -1, -1),
        ])
        remaining_coefficients()

    def forward_rows():
        arrived(bulk + far_source)
        for far in range(1, 5):
            count = HY - far if far > 1 else HY - 2
            low_row, high_row = far, last + 1 + (1 if far == 1 else 0)
            for w in (LZ - far, 2 * LZ - 1 + far):
                forwarded.append(push(f.at[w, rows_of(low_row + ROWS, count)], f.at[w, rows_of(low_row, count)], 0, 1))
                forwarded.append(push(f.at[w, rows_of(high_row - ROWS, count)], f.at[w, rows_of(high_row, count)], 0, -1))

    def presmooth_window():
        arrived(forwarded)
        sent(later)
        start_from_zero(v0, all_layers, 0, NYW)
        sweep(v0, v1, inner, 1, NYW - 1)

    coarse_cycle(0, background_one, forward_rows, presmooth_window)
    arrived(later)
    correct(all_layers, H1 - 1, H1 + 5, (1, NYW - 2), lambda w, y: v1[w, rows_of(y), :], v1)
    bufs = (v1, v0)
    for s in range(4):
        sweep(bufs[s % 2], bufs[(s + 1) % 2], list(range(s + 1, NW - 1 - s)), s + 2, NYW - 2 - s)
    restricted_residual(v1, 1)

    tail = []

    def background_two():
        tail.extend([
            push(v1.at[pl.ds(5, 3), own], v2.at[pl.ds(1, 3), own], 1, 0),
            push(v1.at[pl.ds(4, 3), own], v2.at[pl.ds(8, 3), own], -1, 0),
            push(v1.at[pl.ds(4, 4), rows_of(last - 2, 3)], v2.at[pl.ds(4, 4), rows_of(HY - 3, 3)], 0, 1),
            push(v1.at[pl.ds(4, 4), rows_of(HY, 3)], v2.at[pl.ds(4, 4), rows_of(last + 1, 3)], 0, -1),
            push(v1.at[pl.ds(6, 2), rows_of(last - 1, 2)], v2.at[pl.ds(2, 2), rows_of(HY - 2, 2)], 1, 1),
            push(v1.at[pl.ds(6, 2), rows_of(HY, 2)], v2.at[pl.ds(2, 2), rows_of(last + 1, 2)], 1, -1),
            push(v1.at[pl.ds(4, 2), rows_of(last - 1, 2)], v2.at[pl.ds(8, 2), rows_of(HY - 2, 2)], -1, 1),
            push(v1.at[pl.ds(4, 2), rows_of(HY, 2)], v2.at[pl.ds(8, 2), rows_of(last + 1, 2)], -1, -1),
        ])

    coarse_cycle(1, background_two, lambda: None, lambda: None)
    arrived(tail)

    def keep_own(y):
        for w in own_layers:
            v2[w, rows_of(y), :] = v1[w, rows_of(y), :]

    row_loop(HY, HY + ROWS, 4, keep_own)
    deep = list(range(1, NW - 1))
    correct(deep, H1 - 1, H1 + 5, (), lambda w, y: v2[w, rows_of(y), :], v0)
    sent(tail)
    sweep(v0, v1, deep[1:-1], HY - 2, HY + ROWS + 2)
    sweep(v1, v0, deep[2:-2], HY - 1, HY + ROWS + 1)

    consts, _ = layer_consts(own_layers)

    def defect(y):
        for w in own_layers:
            x, total = flows(v0, w, y, consts[w])
            v2[w, rows_of(y), :] = total - diagonal(w, y, consts[w]) * x

    row_loop(HY, HY + ROWS, 4, defect)

    for k in range(K):
        block = jnp.concatenate([src[w, pl.ds(HY * K + k, ROWS, stride=K), :]
                                 for src in (v0, v2) for w in own_layers], axis=0)
        out[pl.ds(k, LANES, stride=K), :] = block.T
    sent(par + near + bulk + far_source + forwarded)


def natural(turned, v_out, b_out):
    for m in range(turned.shape[0] // LANES):
        block = turned[m * LANES:(m + 1) * LANES, :].T
        v_out[:, :, m * LANES:(m + 1) * LANES] = block[0:LZ * ROWS].reshape(LZ, ROWS, LANES)
        b_out[:, :, m * LANES:(m + 1) * LANES] = block[LZ * ROWS:].reshape(LZ, ROWS, LANES)


N_COPIES = 3 + 8 + 2 + 8 + 16 + 8 + 2 * (3 + 6 + 2 * H2)


def local(n_tile, source_heating, material_thermal_values, layer_material, via_conductance, via_blocks):
    def tiles(*lead):
        return pltpu.VMEM(lead + (NZ, LANES), F32)

    def window(n):
        return pltpu.VMEM((n, NYW * K, LANES), F32)

    vmem = pl.BlockSpec(memory_space=pltpu.VMEM)
    smem = pl.BlockSpec(memory_space=pltpu.SMEM)
    shape = jax.ShapeDtypeStruct(source_heating.shape, F32)
    turned = pl.pallas_call(
        functools.partial(kernel, n_tile),
        out_shape=jax.ShapeDtypeStruct((K * LANES, LANES), F32),
        in_specs=[pl.BlockSpec(memory_space=pl.ANY), smem, smem, smem, vmem],
        out_specs=vmem,
        scratch_shapes=[
            pltpu.VMEM(source_heating.shape, F32),
            window(NW), window(NW), window(NW), window(NW), window(4),
            pltpu.VMEM((NYW * K, LANES), F32), window(3), window(3),
            pltpu.VMEM((4, 8, LANES), F32), tiles(2),
            pltpu.VMEM((K * LANES, LANES), F32), pltpu.VMEM((4 * 6 * K, LANES), F32),
            pltpu.VMEM((2, 4, 12, 8, LANES), F32), tiles(2, N1 * 4),
            tiles(N1 * 4), tiles(N1 * 4), tiles(N1 * 4), tiles(N1 * 4), tiles(N1 * 4),
            tiles(2, N2), tiles(N2), tiles(N2), tiles(N2), tiles(N2), tiles(N2),
            pltpu.VMEM((4, 80, LANES), F32), pltpu.VMEM((8, LANES), F32),
            pltpu.SemaphoreType.DMA((N_COPIES,)),
            pltpu.SemaphoreType.DMA((N_COPIES,)),
            pltpu.SemaphoreType.DMA((4,)),
        ],
        compiler_params=pltpu.CompilerParams(collective_id=0, has_side_effects=True),
    )(source_heating, material_thermal_values, layer_material, via_conductance, via_blocks.transpose(0, 2, 1))
    steps = 4
    chunk = K * LANES // steps
    whole = pl.BlockSpec((LZ, ROWS, chunk), lambda i: (0, 0, i))
    return pl.pallas_call(
        natural,
        grid=(steps,),
        out_shape=(shape, shape),
        in_specs=[pl.BlockSpec((chunk, LANES), lambda i: (i, 0))],
        out_specs=(whole, whole),
    )(turned)


def solution(mesh):
    in_specs = (P("die", "tile", None), P(), P("die"), P("die"), P("die", None, None))
    out_specs = (P("die", "tile", None), P("die", "tile", None))
    body = functools.partial(local, mesh.shape["tile"])
    return jax.shard_map(body, mesh=mesh, in_specs=in_specs, out_specs=out_specs, check_vma=False)
```

```python
import functools

import jax
import jax.numpy as jnp
from jax import lax
from jax.experimental import pallas as pl
from jax.experimental.pallas import tpu as pltpu
from jax.sharding import PartitionSpec as P

F32 = jnp.float32
OMEGA = 0.8
KEEP = 1.0 - OMEGA
LZ = 4
ROWS = 16
HY = 6
NYW = ROWS + 2 * HY
NW = 3 * LZ
K = 16
LANES = 128
H1 = 5
N1 = 4 + 2 * H1
H2 = 6
N2 = 1 + 2 * H2
NZ = 16


def rows_of(y, count=1):
    start = y * K
    if not isinstance(start, int):
        start = pl.multiple_of(start, K)
    return pl.ds(start, count * K)


def row_loop(lo, hi, unroll, fn):
    whole = (hi - lo) // unroll

    def body(i, carry):
        for j in range(unroll):
            fn(lo + i * unroll + j)
        return carry

    if whole:
        lax.fori_loop(0, whole, body, 0)
    for y in range(lo + whole * unroll, hi):
        fn(y)


def kernel(n_tile, f_in, mats_in, material_in, via_cond_in, blocks_in, out, mats, material, via_cond, blocks, f_vm, f, v0, v1, v2, vn, vd_top, wlo, whi, pall, cz,
           turn, restr, r1g, r1, w1, u1, l1, a1, b1, r2, w2, u2, l2, a2, b2, via1, pk, send_sem, recv_sem, in_sem):
    d = lax.axis_index("die")
    t = lax.axis_index("tile")

    def at(dd, dt):
        return {"die": lax.rem(d + dd + 4, 4), "tile": lax.rem(t + dt + n_tile, n_tile)}

    counter = [0]

    def push(src, dst, dd, dt):
        i = counter[0]
        counter[0] += 1
        copy = pltpu.make_async_remote_copy(
            src_ref=src, dst_ref=dst, send_sem=send_sem.at[i], recv_sem=recv_sem.at[i],
            device_id=at(dd, dt), device_id_type=pl.DeviceIdType.MESH)
        copy.start()
        return copy

    def arrived(copies):
        for copy in copies:
            copy.wait_recv()

    def sent(copies):
        for copy in copies:
            copy.wait_send()

    loads = []
    for g in range(4):
        part = (slice(None), slice(None), pl.ds(g * 4 * LANES, 4 * LANES))
        loads.append(pltpu.make_async_copy(f_in.at[part], f_vm.at[part], in_sem.at[g]))
        loads[g].start()

    small = []
    for g, (src, dst) in enumerate(((mats_in, mats), (material_in, material), (via_cond_in, via_cond), (blocks_in, blocks))):
        small.append(pltpu.make_async_copy(src, dst, in_sem.at[4 + g]))
        small[g].start()

    partners = [(1, 0), (2, 0), (3, 0), (1, 1), (1, -1), (-1, 1), (-1, -1)]
    partners += [(0, s * j) for j in range(1, H2 + 1) for s in (1, -1)]
    barrier = pltpu.get_barrier_semaphore()
    for dd, dt in partners:
        pl.semaphore_signal(barrier, inc=1, device_id=at(dd, dt), device_id_type=pl.DeviceIdType.MESH)

    for g in range(4):
        loads[g].wait()
        for m in range(4 * g, 4 * g + 4):
            block = f_vm[:, :, m * LANES:(m + 1) * LANES].reshape(LZ * ROWS, LANES)
            turn[m * LANES:(m + 1) * LANES, 0:LZ * ROWS] = block.T
    for k in range(K):
        block = turn[pl.ds(k, LANES, stride=K), 0:LZ * ROWS].T
        for z in range(LZ):
            f[LZ + z, pl.ds(HY * K + k, ROWS, stride=K), :] = block[z * ROWS:(z + 1) * ROWS]
    zero_row = jnp.zeros((K, LANES), F32)

    def clear(y):
        for w in (0, 1, NW - 2, NW - 1):
            v1[w, rows_of(y), :] = zero_row

    row_loop(0, NYW, 4, clear)

    for copy in small:
        copy.wait()
    pk[0:4, :] = jnp.full((4, LANES), via_cond[0], F32)
    pk[0:4, 0:24] = blocks[0].astype(F32)
    for z in range(LZ):
        pk[4 + z:5 + z, :] = jnp.full((1, LANES), mats[material[z]], F32)
    pall[d] = pk[...]

    def coverage(e, rows, row0, cell, lanes_cols):
        n_lanes = lanes_cols * LANES
        prm = pall[e]
        down = prm.T
        lane = lax.broadcasted_iota(jnp.int32, (24, n_lanes), 1)
        col = (((lane & (LANES - 1)) * lanes_cols + (lane >> 7)) * cell).astype(F32)
        c_lo, c_hi = down[0:24, 1:2], down[0:24, 1:2] + down[0:24, 3:4]
        cols = jnp.maximum(jnp.minimum(c_hi, col + cell) - jnp.maximum(c_lo, col), 0.0)
        row = ((row0 + lax.broadcasted_iota(jnp.int32, (rows, LANES), 0)) * cell).astype(F32)
        r_lo, r_hi = prm[0:1, :], prm[0:1, :] + prm[2:3, :]
        cover = jnp.maximum(jnp.minimum(r_hi, row + cell) - jnp.maximum(r_lo, row), 0.0)
        return jnp.dot(cover[:, 0:24], cols, precision=lax.Precision.HIGHEST,
                       preferred_element_type=F32) * prm[0:1, LANES - 1:]

    zs = lax.broadcasted_iota(jnp.int32, (NZ, LANES), 0)
    is_top = (zs & 3) == 3
    is_end = zs == NZ - 1
    lanes8 = lax.broadcasted_iota(jnp.int32, (8, LANES), 1)
    subs8 = lax.broadcasted_iota(jnp.int32, (8, LANES), 0)
    lanes16 = lax.broadcasted_iota(jnp.int32, (NZ, LANES), 1)

    def valid(row, count):
        return jnp.where((row >= 0) & (row < count), 1.0, 0.0).astype(F32)

    def fine_valid(y):
        return valid(t * ROWS - HY + y, n_tile * ROWS)

    def via_plane(j):
        plane = coverage(lax.rem(d + 2 + j, 4), 32, t * ROWS - HY, 1, K)
        for k in range(K):
            vn[j, pl.ds(k, NYW, stride=K), :] = plane[0:NYW, k * LANES:(k + 1) * LANES]

    via_plane(2)
    pl.semaphore_wait(barrier, len(partners))

    own = rows_of(HY, ROWS)
    last = HY + ROWS - 1
    par = [push(pk, pall.at[d], dd, 0) for dd in (1, 2, 3)]
    near = [
        push(f.at[7, own], f.at[3, own], 1, 0),
        push(f.at[4, own], f.at[8, own], -1, 0),
        push(f.at[pl.ds(4, 4), rows_of(last + 1 - HY, HY)], f.at[pl.ds(4, 4), rows_of(0, HY)], 0, 1),
        push(f.at[pl.ds(4, 4), rows_of(HY, HY)], f.at[pl.ds(4, 4), rows_of(HY + ROWS, HY)], 0, -1),
        push(f.at[7, rows_of(last)], f.at[3, rows_of(HY - 1)], 1, 1),
        push(f.at[7, rows_of(HY)], f.at[3, rows_of(last + 1)], 1, -1),
        push(f.at[4, rows_of(last)], f.at[8, rows_of(HY - 1)], -1, 1),
        push(f.at[4, rows_of(HY)], f.at[8, rows_of(last + 1)], -1, -1),
    ]
    bulk = [
        push(f.at[6, own], f.at[2, own], 1, 0),
        push(f.at[5, own], f.at[9, own], -1, 0),
        push(f.at[5, rows_of(HY, 8)], f.at[1, rows_of(HY, 8)], 1, 0),
        push(f.at[6, rows_of(HY, 8)], f.at[10, rows_of(HY, 8)], -1, 0),
    ]

    def clear_v2(y):
        for w in range(NW):
            v2[w, rows_of(y), :] = zero_row

    row_loop(0, NYW, 2, clear_v2)
    arrived(par)
    via_plane(1)

    cond = jnp.concatenate([pall[e, 4:8, :] for e in range(4)], axis=0)
    follow = jnp.concatenate([cond[1:], cond[NZ - 1:]], axis=0)
    vert = 2.0 * cond * follow / (cond + follow)
    cz[0] = cond
    cz[1] = vert

    def zrow(which, w):
        z = lax.rem(LZ * (d + 3) + w, NZ)
        return cz[which, pl.ds(z, 1), :]

    def splat(w):
        ty = w % LZ
        c = zrow(0, w)
        u = zrow(1, w) if ty < 3 else None
        lo = zrow(1, w - 1) if ty > 0 else None
        return c, u, lo

    edge = [jnp.where(lax.rem(d + 2 + j, 4) == 3, 0.0, 1.0).astype(F32) for j in range(4)]
    ends = [(splat(LZ * m), splat(LZ * m + 3)) for m in range(3)]

    def weight_below(m, y, ok, coupled):
        c, u, _ = ends[m][0]
        wlo[m, rows_of(y), :] = ok / (4.0 * c + u + coupled)

    def weight_above(m, y, ok, plane):
        c, _, lo = ends[m][1]
        whi[m, rows_of(y), :] = ok / (4.0 * c + lo + plane)

    def near_weights(y):
        ok = fine_valid(y) * OMEGA
        planes = {j: vn[j, rows_of(y), :] for j in (1, 2)}
        vd_top[rows_of(y), :] = planes[2]
        for j in (1, 2):
            coupled = planes[j] * edge[j]
            vn[j, rows_of(y), :] = coupled
            weight_below(j, y, ok, coupled)
            weight_above(j - 1, y, ok, planes[j])

    row_loop(0, NYW, 4, near_weights)

    def far_weights(y):
        ok = fine_valid(y) * OMEGA
        planes = {j: vn[j, rows_of(y), :] for j in (0, 3)}
        for j in (0, 3):
            vn[j, rows_of(y), :] = planes[j] * edge[j]
        weight_below(0, y, ok, planes[0] * edge[0])
        weight_above(2, y, ok, planes[3])

    def coarse_coeffs(via_rows, scale, couple, row_ok):
        via = jnp.zeros((NZ, LANES), F32)
        for e in range(4):
            via = jnp.where(zs == LZ * e + 3, via_rows[e], via)
        upper = jnp.where(is_top, via, vert * couple)
        nb = jnp.where(is_end, 0.0, upper)
        lower = pltpu.roll(nb, 1, 0)
        return (row_ok * OMEGA) / (4.0 * scale * cond + upper + lower), nb, lower

    def mid_coeffs(i):
        ok = valid(t * 4 - H1 + i, n_tile * 4)
        for p in range(4):
            got = coarse_coeffs([via1[e, pl.ds(p * 16 + i, 1), :] for e in range(4)], 4.0, 16.0, ok)
            w1[i * 4 + p], u1[i * 4 + p], l1[i * 4 + p] = got

    def low_coeffs(i):
        ok = valid(t - H2 + i, n_tile)
        got = coarse_coeffs([via1[e, pl.ds(64 + i, 1), :] for e in range(4)], 16.0, 256.0, ok)
        w2[i], u2[i], l2[i] = got

    def remaining_coefficients():
        for e in range(4):
            plane = coverage(e, 16, t * 4 - H1, 4, 4)
            for p in range(4):
                via1[e, p * 16:(p + 1) * 16, :] = plane[:, p * LANES:(p + 1) * LANES]
            via1[e, 64:80, :] = coverage(e, 16, t - H2, 16, 1)
        row_loop(0, N1, 2, mid_coeffs)
        row_loop(0, N2, 4, low_coeffs)
        via_plane(0)
        via_plane(3)
        row_loop(0, NYW, 4, far_weights)

    def beside(x):
        nxt = pltpu.roll(x, K - 1, 0)
        prv = pltpu.roll(x, 1, 0)
        n_lo, n_hi = nxt[0:8], nxt[8:16]
        p_lo, p_hi = prv[0:8], prv[8:16]
        n_in = jnp.where(lanes8 == LANES - 1, 0.0, pltpu.roll(n_hi, LANES - 1, 1))
        p_in = jnp.where(lanes8 == 0, 0.0, pltpu.roll(p_lo, 1, 1))
        n_hi = jnp.where(subs8 == 7, n_in, n_hi)
        p_lo = jnp.where(subs8 == 0, p_in, p_lo)
        return jnp.concatenate([n_lo + p_lo, n_hi + p_hi], axis=0)

    def flows(src, w, y, consts, above=True, below=True):
        c, u, lo = consts
        ty, m = w % LZ, w // LZ
        x = src[w, rows_of(y), :]
        side = (src[w, rows_of(y - 1), :] + src[w, rows_of(y + 1), :]) + beside(x)
        total = f[w, rows_of(y), :] + c * side
        if above:
            total += (vn[m + 1, rows_of(y), :] if ty == 3 else u) * src[w + 1, rows_of(y), :]
        if below:
            total += (vn[m, rows_of(y), :] if ty == 0 else lo) * src[w - 1, rows_of(y), :]
        return x, total

    def plain_weight(consts):
        c, u, lo = consts
        return OMEGA / (4.0 * c + u + lo)

    def weight(w, y, plain):
        ty, m = w % LZ, w // LZ
        if ty == 0:
            return wlo[m, rows_of(y), :]
        if ty == 3:
            return whi[m, rows_of(y), :]
        return plain * fine_valid(y)

    def layer_consts(layers):
        consts = {w: splat(w) for w in layers}
        plain = {w: plain_weight(consts[w]) for w in layers if w % LZ in (1, 2)}
        return consts, plain

    def start_from_zero(dst, layers, y_lo, y_hi):
        _, plain = layer_consts(layers)

        def body(y):
            for w in layers:
                dst[w, rows_of(y), :] = weight(w, y, plain.get(w)) * f[w, rows_of(y), :]

        row_loop(y_lo, y_hi, max(1, 16 // len(layers)), body)

    def unroll_of(layers, rows):
        return max(u for u in (1, 2, 3, 4, 6) if rows % u == 0 and u * len(layers) <= 24)

    def sweep(src, dst, layers, y_lo, y_hi):
        consts, plain = layer_consts(layers)

        def body(y):
            for w in layers:
                x, total = flows(src, w, y, consts[w])
                dst[w, rows_of(y), :] = KEEP * x + weight(w, y, plain.get(w)) * total

        row_loop(y_lo, y_hi, unroll_of(layers, y_hi - y_lo), body)

    def diagonal(w, y, consts):
        c, u, lo = consts
        if w == LZ:
            return 4.0 * c + u + vn[1, rows_of(y), :]
        if w == LZ + 3:
            return 4.0 * c + lo + vd_top[rows_of(y), :]
        return 4.0 * c + u + lo

    own_layers = list(range(LZ, 2 * LZ))

    def restricted_residual(src, slot):
        consts, _ = layer_consts(own_layers)

        def body(i, carry):
            sums = [None] * 6
            for q in range(4):
                y = HY + i * 4 + q
                parts = []
                for w in own_layers:
                    x, total = flows(src, w, y, consts[w], above=w < LZ + 3, below=w > LZ)
                    parts.append(total - diagonal(w, y, consts[w]) * x)
                parts.append(vn[1, rows_of(y), :] * src[LZ, rows_of(y), :])
                parts.append(vn[2, rows_of(y), :] * src[LZ + 3, rows_of(y), :])
                sums = [p if s is None else s + p for s, p in zip(sums, parts)]
            for s in range(4):
                restr[pl.ds(pl.multiple_of((i * 4 + s) * K, K), K), :] = sums[s]
            for s in range(2):
                restr[pl.ds(pl.multiple_of(16 * K + (i * 2 + s) * K, K), K), :] = sums[4 + s]
            return carry

        lax.fori_loop(0, 4, body, 0)
        for g, start in enumerate((0, 16 * K, 8 * K)):
            for p in range(4):
                tile = restr[pl.ds(start + 4 * p, 8, stride=K), :]
                for q in range(1, 4):
                    tile += restr[pl.ds(start + 4 * p + q, 8, stride=K), :]
                r1g[slot, d, g * 4 + p] = tile

    mid_c = 4.0 * cond
    low_c = 16.0 * cond

    def lane_next(x):
        return jnp.where(lanes16 == LANES - 1, 0.0, pltpu.roll(x, LANES - 1, 1))

    def lane_prev(x):
        return jnp.where(lanes16 == 0, 0.0, pltpu.roll(x, 1, 1))

    def mid_flows(src, rhs, i):
        xs = [src[i * 4 + p] for p in range(4)]
        out = []
        for p in range(4):
            nxt = xs[p + 1] if p < 3 else lane_next(xs[0])
            prv = xs[p - 1] if p > 0 else lane_prev(xs[3])
            side = (src[i * 4 - 4 + p] + src[i * 4 + 4 + p]) + (nxt + prv)
            total = rhs[i * 4 + p] + mid_c * side
            total += u1[i * 4 + p] * pltpu.roll(xs[p], NZ - 1, 0)
            total += l1[i * 4 + p] * pltpu.roll(xs[p], 1, 0)
            out.append((xs[p], total))
        return out

    def mid_sweep(src, dst, rhs, lo, hi):
        def body(i):
            for p, (x, total) in enumerate(mid_flows(src, rhs, i)):
                dst[i * 4 + p] = KEEP * x + w1[i * 4 + p] * total

        row_loop(lo, hi, max(u for u in (1, 2, 3, 4, 5) if (hi - lo) % u == 0), body)

    def mid_start(rhs, lo, hi):
        def body(i):
            for p in range(4):
                a1[i * 4 + p] = w1[i * 4 + p] * rhs[i * 4 + p]

        row_loop(lo, hi, 2, body)

    def assemble(slot):
        def turned(x, shift):
            return x if shift % 8 == 0 else pltpu.roll(x, shift % 8, 0)

        for i in range(4):
            half = 4 * (i % 2)
            for p in range(4):
                ts = [r1g[slot, e, (0 if i < 2 else 8) + p] for e in range(4)]
                cs = [r1g[slot, e, 4 + p] for e in range(4)]

                def put(e, down, dst_row):
                    return jnp.where(subs8 == dst_row, turned(cs[e], dst_row - (2 * i + down)), 0.0)

                lo = jnp.where(subs8 < 4, turned(ts[0], -half), turned(ts[1], 4 - half))
                lo += put(1, 0, 3) + put(0, 1, 4) + put(2, 0, 7)
                hi = jnp.where(subs8 < 4, turned(ts[2], -half), turned(ts[3], 4 - half))
                hi += put(1, 1, 0) + put(3, 0, 3) + put(2, 1, 4)
                r1[slot, (H1 + i) * 4 + p] = jnp.concatenate([lo, hi], axis=0)

    def coarse_cycle(slot, after_gather, after_spread, while_waiting):
        gather = [push(r1g.at[slot, d], r1g.at[slot, d], dd, 0) for dd in (2, 1, 3)]
        after_gather()
        arrived(gather)
        assemble(slot)
        rhs = r1.at[slot]

        def mid_rows(i, count):
            return rhs.at[pl.ds(i * 4, count * 4)]

        urgent = [
            push(mid_rows(H1 + 2, 2), mid_rows(H1 - 2, 2), 0, 1),
            push(mid_rows(H1, 2), mid_rows(H1 + 4, 2), 0, -1),
        ]
        rest = [
            push(mid_rows(H1, 2), mid_rows(H1 - 4, 2), 0, 1),
            push(mid_rows(H1 + 2, 2), mid_rows(H1 + 6, 2), 0, -1),
            push(mid_rows(H1 + 3, 1), mid_rows(0, 1), 0, 2),
            push(mid_rows(H1, 1), mid_rows(N1 - 1, 1), 0, -2),
        ]
        after_spread()
        arrived(urgent)
        mid_start(rhs, H1 - 2, H1 + 6)
        mid_sweep(a1, b1, rhs, H1 - 1, H1 + 5)

        def down(i, acc):
            for j in range(2):
                row = H1 + 2 * i + j
                for p, (x, total) in enumerate(mid_flows(b1, rhs, row)):
                    acc += total - (OMEGA / w1[row * 4 + p]) * x
            return acc

        r2[slot, H2] = lax.fori_loop(0, 2, down, jnp.zeros((NZ, LANES), F32))
        low = []
        for j in range(H2, 0, -1):
            low.append(push(r2.at[slot, H2], r2.at[slot, H2 - j], 0, j))
            low.append(push(r2.at[slot, H2], r2.at[slot, H2 + j], 0, -j))
        arrived(rest)
        mid_start(rhs, 0, H1 - 2)
        mid_start(rhs, H1 + 6, N1)
        mid_sweep(a1, b1, rhs, 1, H1 - 1)
        mid_sweep(a1, b1, rhs, H1 + 5, N1 - 1)
        while_waiting()
        arrived(low)

        bufs = (a2, b2)
        for i in range(N2):
            a2[i] = w2[i] * r2[slot, i]
        for s in range(5):
            src, dst = bufs[s % 2], bufs[(s + 1) % 2]
            for i in range(s + 1, N2 - 1 - s):
                x = src[i]
                side = (src[i - 1] + src[i + 1]) + (lane_next(x) + lane_prev(x))
                total = r2[slot, i] + low_c * side
                total += u2[i] * pltpu.roll(x, NZ - 1, 0) + l2[i] * pltpu.roll(x, 1, 0)
                dst[i] = KEEP * x + w2[i] * total
        fix = bufs[1]
        for g in range(3):
            e2 = fix[H2 - 1 + g]
            for i in range(4):
                for p in range(4):
                    at_cell = (H1 - 4 + g * 4 + i) * 4 + p
                    b1[at_cell] = b1[at_cell] + e2
        mid_sweep(b1, a1, rhs, 2, N1 - 2)
        mid_sweep(a1, b1, rhs, 3, N1 - 3)
        sent(gather + urgent + rest + low)

    def correction(i, w):
        z = lax.rem(LZ * (d + 3) + w, NZ)
        rows = [b1[i * 4 + p, pl.ds(z, 1), :] for p in range(4)]
        lo = jnp.where(subs8 < 4, rows[0], rows[1])
        hi = jnp.where(subs8 < 4, rows[2], rows[3])
        return jnp.concatenate([lo, hi], axis=0)

    def correct(layers, i_lo, i_hi, edge_rows, pick, dst):
        def row(i, y, fix, w):
            dst[w, rows_of(y), :] = pick(w, y) * fine_valid(y) + fix

        def body(i):
            for w in layers:
                fix = correction(i, w)
                for q in range(4):
                    row(i, HY + (i - H1) * 4 + q, fix, w)

        row_loop(i_lo, i_hi, 1, body)
        for y in edge_rows:
            i = (y - HY) // 4 + H1
            for w in layers:
                row(i, y, correction(i, w), w)

    arrived(near[2:4])
    start_from_zero(v0, own_layers, HY - 2, HY + ROWS + 2)
    sweep(v0, v1, [5, 6], HY - 1, HY + ROWS + 1)
    arrived(near[0:2] + near[4:])
    start_from_zero(v0, [3, 8], HY - 1, HY + ROWS + 1)
    sweep(v0, v1, [4, 7], HY - 1, HY + ROWS + 1)
    restricted_residual(v1, 0)

    later = []
    forwarded = []
    far_source = []
    all_layers = list(range(NW))
    inner = list(range(1, NW - 1))

    def background_one():
        far_source.extend([
            push(f.at[5, rows_of(HY + 8, 8)], f.at[1, rows_of(HY + 8, 8)], 1, 0),
            push(f.at[6, rows_of(HY + 8, 8)], f.at[10, rows_of(HY + 8, 8)], -1, 0),
        ])
        later.extend([
            push(v1.at[pl.ds(4, 2), own], v1.at[pl.ds(0, 2), own], 1, 0),
            push(v1.at[pl.ds(6, 2), own], v1.at[pl.ds(10, 2), own], -1, 0),
            push(v1.at[pl.ds(4, 2), rows_of(last - 1, 2)], v1.at[pl.ds(0, 2), rows_of(HY - 2, 2)], 1, 1),
            push(v1.at[pl.ds(4, 2), rows_of(HY, 2)], v1.at[pl.ds(0, 2), rows_of(last + 1, 2)], 1, -1),
            push(v1.at[pl.ds(6, 2), rows_of(last - 1, 2)], v1.at[pl.ds(10, 2), rows_of(HY - 2, 2)], -1, 1),
            push(v1.at[pl.ds(6, 2), rows_of(HY, 2)], v1.at[pl.ds(10, 2), rows_of(last + 1, 2)], -1, -1),
        ])
        remaining_coefficients()
        arrived(bulk)
        forward(1)
        forward(2)

    def forward(far):
        count = HY - far if far > 1 else HY - 2
        low_row, high_row = far, last + 1 + (1 if far == 1 else 0)
        for w in (LZ - far, 2 * LZ - 1 + far):
            forwarded.append(push(f.at[w, rows_of(low_row + ROWS, count)], f.at[w, rows_of(low_row, count)], 0, 1))
            forwarded.append(push(f.at[w, rows_of(high_row - ROWS, count)], f.at[w, rows_of(high_row, count)], 0, -1))

    outer = [2, 3, 8, 9]

    def forward_last():
        arrived(far_source)
        forward(3)

    def window_inside():
        start_from_zero(v0, [1, 2, 3, 8, 9, 10], HY, HY + ROWS)
        sweep(v0, v1, outer, HY + 1, HY + ROWS - 1)

    def presmooth_window():
        window_inside()
        arrived(forwarded)
        sent(later)
        for lo, hi in ((0, HY), (HY + ROWS, NYW)):
            start_from_zero(v0, inner, lo, hi)
        sweep(v0, v1, own_layers, 1, HY - 1)
        sweep(v0, v1, own_layers, HY + ROWS + 1, NYW - 1)
        sweep(v0, v1, outer, 1, HY + 1)
        sweep(v0, v1, outer, HY + ROWS - 1, NYW - 1)

    coarse_cycle(0, background_one, forward_last, presmooth_window)
    arrived(later)
    correct(all_layers, H1 - 1, H1 + 5, (1, NYW - 2), lambda w, y: v1[w, rows_of(y), :], v1)
    bufs = (v1, v0)
    for s in range(4):
        sweep(bufs[s % 2], bufs[(s + 1) % 2], list(range(s + 1, NW - 1 - s)), s + 2, NYW - 2 - s)
    restricted_residual(v1, 1)

    tail = []

    def background_two():
        tail.extend([
            push(v1.at[pl.ds(5, 3), own], v2.at[pl.ds(1, 3), own], 1, 0),
            push(v1.at[pl.ds(4, 3), own], v2.at[pl.ds(8, 3), own], -1, 0),
            push(v1.at[pl.ds(4, 4), rows_of(last - 2, 3)], v2.at[pl.ds(4, 4), rows_of(HY - 3, 3)], 0, 1),
            push(v1.at[pl.ds(4, 4), rows_of(HY, 3)], v2.at[pl.ds(4, 4), rows_of(last + 1, 3)], 0, -1),
            push(v1.at[pl.ds(6, 2), rows_of(last - 1, 2)], v2.at[pl.ds(2, 2), rows_of(HY - 2, 2)], 1, 1),
            push(v1.at[pl.ds(6, 2), rows_of(HY, 2)], v2.at[pl.ds(2, 2), rows_of(last + 1, 2)], 1, -1),
            push(v1.at[pl.ds(4, 2), rows_of(last - 1, 2)], v2.at[pl.ds(8, 2), rows_of(HY - 2, 2)], -1, 1),
            push(v1.at[pl.ds(4, 2), rows_of(HY, 2)], v2.at[pl.ds(8, 2), rows_of(last + 1, 2)], -1, -1),
        ])

    coarse_cycle(1, background_two, lambda: None, lambda: None)
    arrived(tail)

    def keep_own(y):
        for w in own_layers:
            v2[w, rows_of(y), :] = v1[w, rows_of(y), :]

    row_loop(HY, HY + ROWS, 4, keep_own)
    deep = list(range(1, NW - 1))
    correct(deep, H1 - 1, H1 + 5, (), lambda w, y: v2[w, rows_of(y), :], v0)
    sent(tail)
    sweep(v0, v1, deep[1:-1], HY - 2, HY + ROWS + 2)
    sweep(v1, v0, deep[2:-2], HY - 1, HY + ROWS + 1)

    consts, _ = layer_consts(own_layers)

    def defect(y):
        for w in own_layers:
            x, total = flows(v0, w, y, consts[w])
            v2[w, rows_of(y), :] = total - diagonal(w, y, consts[w]) * x

    row_loop(HY, HY + ROWS, 4, defect)

    for k in range(K):
        block = jnp.concatenate([src[w, pl.ds(HY * K + k, ROWS, stride=K), :]
                                 for src in (v0, v2) for w in own_layers], axis=0)
        out[pl.ds(k, LANES, stride=K), :] = block.T
    sent(par + near + bulk + far_source + forwarded)


OUT_PARTS = 4


def natural(turned_in, v_out, b_out, turned, v_vm, b_vm, sem):
    copies = []
    per = K // OUT_PARTS
    loads = []
    for g in range(OUT_PARTS):
        part = pl.ds(g * per * LANES, per * LANES)
        loads.append(pltpu.make_async_copy(turned_in.at[part], turned.at[part], sem.at[2, g]))
        loads[g].start()
    for g in range(OUT_PARTS):
        loads[g].wait()
        for m in range(g * per, (g + 1) * per):
            block = turned[m * LANES:(m + 1) * LANES, :].T
            v_vm[:, :, m * LANES:(m + 1) * LANES] = block[0:LZ * ROWS].reshape(LZ, ROWS, LANES)
            b_vm[:, :, m * LANES:(m + 1) * LANES] = block[LZ * ROWS:].reshape(LZ, ROWS, LANES)
        part = (slice(None), slice(None), pl.ds(g * per * LANES, per * LANES))
        for i, (src, dst) in enumerate(((v_vm, v_out), (b_vm, b_out))):
            copies.append(pltpu.make_async_copy(src.at[part], dst.at[part], sem.at[i, g]))
            copies[-1].start()
    for copy in copies:
        copy.wait()


N_COPIES = 3 + 8 + 4 + 8 + 12 + 8 + 2 * (3 + 6 + 2 * H2)


def local(n_tile, source_heating, material_thermal_values, layer_material, via_conductance, via_blocks):
    def tiles(*lead):
        return pltpu.VMEM(lead + (NZ, LANES), F32)

    def window(n):
        return pltpu.VMEM((n, NYW * K, LANES), F32)

    vmem = pl.BlockSpec(memory_space=pltpu.VMEM)
    shape = jax.ShapeDtypeStruct(source_heating.shape, F32)
    turned = pl.pallas_call(
        functools.partial(kernel, n_tile),
        out_shape=jax.ShapeDtypeStruct((K * LANES, LANES), F32),
        in_specs=[pl.BlockSpec(memory_space=pltpu.HBM)] * 5,
        out_specs=vmem,
        scratch_shapes=[
            pltpu.SMEM(material_thermal_values.shape, F32), pltpu.SMEM(layer_material.shape, jnp.int32),
            pltpu.SMEM(via_conductance.shape, F32), pltpu.VMEM((1, 4, via_blocks.shape[1]), jnp.int32),
            pltpu.VMEM(source_heating.shape, F32),
            window(NW), window(NW), window(NW), window(NW), window(4),
            pltpu.VMEM((NYW * K, LANES), F32), window(3), window(3),
            pltpu.VMEM((4, 8, LANES), F32), tiles(2),
            pltpu.VMEM((K * LANES, LANES), F32), pltpu.VMEM((4 * 6 * K, LANES), F32),
            pltpu.VMEM((2, 4, 12, 8, LANES), F32), tiles(2, N1 * 4),
            tiles(N1 * 4), tiles(N1 * 4), tiles(N1 * 4), tiles(N1 * 4), tiles(N1 * 4),
            tiles(2, N2), tiles(N2), tiles(N2), tiles(N2), tiles(N2), tiles(N2),
            pltpu.VMEM((4, 80, LANES), F32), pltpu.VMEM((8, LANES), F32),
            pltpu.SemaphoreType.DMA((N_COPIES,)),
            pltpu.SemaphoreType.DMA((N_COPIES,)),
            pltpu.SemaphoreType.DMA((8,)),
        ],
        compiler_params=pltpu.CompilerParams(collective_id=0, has_side_effects=True),
    )(source_heating, material_thermal_values, layer_material, via_conductance, via_blocks.transpose(0, 2, 1))
    anywhere = pl.BlockSpec(memory_space=pl.ANY)
    return pl.pallas_call(
        natural,
        out_shape=(shape, shape),
        in_specs=[anywhere],
        out_specs=(anywhere, anywhere),
        scratch_shapes=[pltpu.VMEM((K * LANES, LANES), F32), pltpu.VMEM(source_heating.shape, F32), pltpu.VMEM(source_heating.shape, F32),
                        pltpu.SemaphoreType.DMA((3, OUT_PARTS))],
    )(turned)


def solution(mesh):
    in_specs = (P("die", "tile", None), P(), P("die"), P("die"), P("die", None, None))
    out_specs = (P("die", "tile", None), P("die", "tile", None))
    body = functools.partial(local, mesh.shape["tile"])
    return jax.shard_map(body, mesh=mesh, in_specs=in_specs, out_specs=out_specs, check_vma=False)
```

```python
import functools

import jax
import jax.numpy as jnp
from jax import lax
from jax.experimental import pallas as pl
from jax.experimental.pallas import tpu as pltpu
from jax.sharding import PartitionSpec as P

F32 = jnp.float32
OMEGA = 0.8
KEEP = 1.0 - OMEGA
LZ = 4
ROWS = 16
HY = 6
NYW = ROWS + 2 * HY
NW = 3 * LZ
K = 16
LANES = 128
H1 = 5
N1 = 4 + 2 * H1
H2 = 6
N2 = 1 + 2 * H2
NZ = 16
STRIP = 8


def rows_of(y, count=1):
    start = y * K
    if not isinstance(start, int):
        start = pl.multiple_of(start, K)
    return pl.ds(start, count * K)


def row_loop(lo, hi, unroll, fn):
    whole = (hi - lo) // unroll

    def body(i, carry):
        for j in range(unroll):
            fn(lo + i * unroll + j)
        return carry

    if whole:
        lax.fori_loop(0, whole, body, 0)
    for y in range(lo + whole * unroll, hi):
        fn(y)


def strip_loop(lo, hi, unroll, fn):
    whole = (hi - lo) // unroll

    def body(i, carry):
        fn(lo + i * unroll, unroll)
        return carry

    if whole:
        lax.fori_loop(0, whole, body, 0)
    if lo + whole * unroll < hi:
        fn(lo + whole * unroll, hi - lo - whole * unroll)


def kernel(n_tile, f_in, mats_in, material_in, via_cond_in, blocks_in, out, mats, material, via_cond, blocks, f_vm, f, v0, v1, v2, vn, vd_top, wlo, whi, pall, cz,
           turn, restr, r1g, r1, w1, u1, l1, a1, b1, r2, w2, u2, l2, a2, b2, via1, pk, ctab, send_sem, recv_sem, in_sem):
    d = lax.axis_index("die")
    t = lax.axis_index("tile")

    def at(dd, dt):
        return {"die": lax.rem(d + dd + 4, 4), "tile": lax.rem(t + dt + n_tile, n_tile)}

    counter = [0]

    def push(src, dst, dd, dt):
        i = counter[0]
        counter[0] += 1
        copy = pltpu.make_async_remote_copy(
            src_ref=src, dst_ref=dst, send_sem=send_sem.at[i], recv_sem=recv_sem.at[i],
            device_id=at(dd, dt), device_id_type=pl.DeviceIdType.MESH)
        copy.start()
        return copy

    def arrived(copies):
        for copy in copies:
            copy.wait_recv()

    def sent(copies):
        for copy in copies:
            copy.wait_send()

    loads = []
    for g in range(4):
        part = (slice(None), slice(None), pl.ds(g * 4 * LANES, 4 * LANES))
        loads.append(pltpu.make_async_copy(f_in.at[part], f_vm.at[part], in_sem.at[g]))
        loads[g].start()

    small = []
    for g, (src, dst) in enumerate(((mats_in, mats), (material_in, material), (via_cond_in, via_cond), (blocks_in, blocks))):
        small.append(pltpu.make_async_copy(src, dst, in_sem.at[4 + g]))
        small[g].start()

    partners = [(1, 0), (2, 0), (3, 0), (1, 1), (1, -1), (-1, 1), (-1, -1)]
    partners += [(0, s * j) for j in range(1, 5) for s in (1, -1)]
    barrier = pltpu.get_barrier_semaphore()
    for dd, dt in partners:
        pl.semaphore_signal(barrier, inc=1, device_id=at(dd, dt), device_id_type=pl.DeviceIdType.MESH)

    for g in range(4):
        loads[g].wait()
        for m in range(4 * g, 4 * g + 4):
            block = f_vm[:, :, m * LANES:(m + 1) * LANES].reshape(LZ * ROWS, LANES)
            turn[m * LANES:(m + 1) * LANES, 0:LZ * ROWS] = block.T
    for k in range(K):
        block = turn[pl.ds(k, LANES, stride=K), 0:LZ * ROWS].T
        for z in range(LZ):
            f[LZ + z, pl.ds(HY * K + k, ROWS, stride=K), :] = block[z * ROWS:(z + 1) * ROWS]
    zero_row = jnp.zeros((K, LANES), F32)

    def clear(y):
        for w in (0, 1, NW - 2, NW - 1):
            v1[w, rows_of(y), :] = zero_row

    row_loop(0, NYW, 4, clear)

    for copy in small:
        copy.wait()
    pk[0:4, :] = jnp.full((4, LANES), via_cond[0], F32)
    pk[0:4, 0:24] = blocks[0].astype(F32)
    for z in range(LZ):
        pk[4 + z:5 + z, :] = jnp.full((1, LANES), mats[material[z]], F32)
    pall[d] = pk[...]

    def coverage(e, rows, row0, cell, lanes_cols):
        n_lanes = lanes_cols * LANES
        prm = pall[e]
        down = prm.T
        lane = lax.broadcasted_iota(jnp.int32, (24, n_lanes), 1)
        col = (((lane & (LANES - 1)) * lanes_cols + (lane >> 7)) * cell).astype(F32)
        c_lo, c_hi = down[0:24, 1:2], down[0:24, 1:2] + down[0:24, 3:4]
        cols = jnp.maximum(jnp.minimum(c_hi, col + cell) - jnp.maximum(c_lo, col), 0.0)
        row = ((row0 + lax.broadcasted_iota(jnp.int32, (rows, LANES), 0)) * cell).astype(F32)
        r_lo, r_hi = prm[0:1, :], prm[0:1, :] + prm[2:3, :]
        cover = jnp.maximum(jnp.minimum(r_hi, row + cell) - jnp.maximum(r_lo, row), 0.0)
        return jnp.dot(cover[:, 0:24], cols, precision=lax.Precision.HIGHEST,
                       preferred_element_type=F32) * prm[0:1, LANES - 1:]

    zs = lax.broadcasted_iota(jnp.int32, (NZ, LANES), 0)
    is_top = (zs & 3) == 3
    is_end = zs == NZ - 1
    lanes8 = lax.broadcasted_iota(jnp.int32, (8, LANES), 1)
    subs8 = lax.broadcasted_iota(jnp.int32, (8, LANES), 0)
    lanes16 = lax.broadcasted_iota(jnp.int32, (NZ, LANES), 1)

    def valid(row, count):
        return jnp.where((row >= 0) & (row < count), 1.0, 0.0).astype(F32)

    def fine_valid(y):
        return valid(t * ROWS - HY + y, n_tile * ROWS)

    def via_plane(j):
        plane = coverage(lax.rem(d + 2 + j, 4), 32, t * ROWS - HY, 1, K)
        for k in range(K):
            vn[j, pl.ds(k, NYW, stride=K), :] = plane[0:NYW, k * LANES:(k + 1) * LANES]

    pl.semaphore_wait(barrier, len(partners))

    own = rows_of(HY, ROWS)
    last = HY + ROWS - 1
    par = [push(pk, pall.at[d], dd, 0) for dd in (1, 2, 3)]
    near = [
        push(f.at[7, own], f.at[3, own], 1, 0),
        push(f.at[4, own], f.at[8, own], -1, 0),
        push(f.at[pl.ds(4, 4), rows_of(last + 1 - HY, HY)], f.at[pl.ds(4, 4), rows_of(0, HY)], 0, 1),
        push(f.at[pl.ds(4, 4), rows_of(HY, HY)], f.at[pl.ds(4, 4), rows_of(HY + ROWS, HY)], 0, -1),
        push(f.at[7, rows_of(last)], f.at[3, rows_of(HY - 1)], 1, 1),
        push(f.at[7, rows_of(HY)], f.at[3, rows_of(last + 1)], 1, -1),
        push(f.at[4, rows_of(last)], f.at[8, rows_of(HY - 1)], -1, 1),
        push(f.at[4, rows_of(HY)], f.at[8, rows_of(last + 1)], -1, -1),
    ]
    bulk = [
        push(f.at[6, own], f.at[2, own], 1, 0),
        push(f.at[5, own], f.at[9, own], -1, 0),
        push(f.at[5, rows_of(HY, 8)], f.at[1, rows_of(HY, 8)], 1, 0),
        push(f.at[6, rows_of(HY, 8)], f.at[10, rows_of(HY, 8)], -1, 0),
    ]

    def clear_v2(y):
        for w in range(NW):
            v2[w, rows_of(y), :] = zero_row

    row_loop(0, NYW, 2, clear_v2)
    via_plane(2)
    arrived(par)
    via_plane(1)

    cond = jnp.concatenate([pall[e, 4:8, :] for e in range(4)], axis=0)
    follow = jnp.concatenate([cond[1:], cond[NZ - 1:]], axis=0)
    vert = 2.0 * cond * follow / (cond + follow)
    cz[0] = cond
    cz[1] = vert

    def zrow(which, w):
        z = lax.rem(LZ * (d + 3) + w, NZ)
        return cz[which, pl.ds(z, 1), :]

    def splat(w):
        ty = w % LZ
        c = zrow(0, w)
        u = zrow(1, w) if ty < 3 else None
        lo = zrow(1, w - 1) if ty > 0 else None
        return c, u, lo

    edge = [jnp.where(lax.rem(d + 2 + j, 4) == 3, 0.0, 1.0).astype(F32) for j in range(4)]
    ends = [(splat(LZ * m), splat(LZ * m + 3)) for m in range(3)]

    def weight_below(m, y, ok, coupled):
        c, u, _ = ends[m][0]
        wlo[m, rows_of(y), :] = ok / (4.0 * c + u + coupled)

    def weight_above(m, y, ok, plane):
        c, _, lo = ends[m][1]
        whi[m, rows_of(y), :] = ok / (4.0 * c + lo + plane)

    def near_weights(y):
        ok = fine_valid(y) * OMEGA
        planes = {j: vn[j, rows_of(y), :] for j in (1, 2)}
        vd_top[rows_of(y), :] = planes[2]
        for j in (1, 2):
            coupled = planes[j] * edge[j]
            vn[j, rows_of(y), :] = coupled
            weight_below(j, y, ok, coupled)
            weight_above(j - 1, y, ok, planes[j])

    row_loop(0, NYW, 4, near_weights)

    def far_weights(y):
        ok = fine_valid(y) * OMEGA
        planes = {j: vn[j, rows_of(y), :] for j in (0, 3)}
        for j in (0, 3):
            vn[j, rows_of(y), :] = planes[j] * edge[j]
        weight_below(0, y, ok, planes[0] * edge[0])
        weight_above(2, y, ok, planes[3])

    def coarse_coeffs(via_rows, scale, couple, row_ok):
        via = jnp.zeros((NZ, LANES), F32)
        for e in range(4):
            via = jnp.where(zs == LZ * e + 3, via_rows[e], via)
        upper = jnp.where(is_top, via, vert * couple)
        nb = jnp.where(is_end, 0.0, upper)
        lower = pltpu.roll(nb, 1, 0)
        return (row_ok * OMEGA) / (4.0 * scale * cond + upper + lower), nb, lower

    def mid_coeffs(i):
        ok = valid(t * 4 - H1 + i, n_tile * 4)
        for p in range(4):
            got = coarse_coeffs([via1[e, pl.ds(p * 16 + i, 1), :] for e in range(4)], 4.0, 16.0, ok)
            w1[i * 4 + p], u1[i * 4 + p], l1[i * 4 + p] = got

    def low_coeffs(i):
        ok = valid(t - H2 + i, n_tile)
        got = coarse_coeffs([via1[e, pl.ds(64 + i, 1), :] for e in range(4)], 16.0, 256.0, ok)
        w2[i], u2[i], l2[i] = got

    def remaining_coefficients():
        for e in range(4):
            plane = coverage(e, 16, t * 4 - H1, 4, 4)
            for p in range(4):
                via1[e, p * 16:(p + 1) * 16, :] = plane[:, p * LANES:(p + 1) * LANES]
            via1[e, 64:80, :] = coverage(e, 16, t - H2, 16, 1)
        row_loop(0, N1, 2, mid_coeffs)
        row_loop(0, N2, 4, low_coeffs)
        via_plane(0)
        via_plane(3)
        row_loop(0, NYW, 4, far_weights)

    def beside(src, w, y):
        base = y * K if isinstance(y, int) else pl.multiple_of(y * K, K)
        first = jnp.broadcast_to(src[w, pl.ds(base, 1), :], (8, LANES))
        final = jnp.broadcast_to(src[w, pl.ds(base + K - 1, 1), :], (8, LANES))
        n_in = jnp.where(lanes8 == LANES - 1, 0.0, pltpu.roll(first, LANES - 1, 1))
        p_in = jnp.where(lanes8 == 0, 0.0, pltpu.roll(final, 1, 1))
        n_hi = jnp.where(subs8 == 7, n_in, src[w, pl.ds(base + 9, 8), :])
        p_lo = jnp.where(subs8 == 0, p_in, src[w, pl.ds(base - 1, 8), :])
        lo = src[w, pl.ds(base + 1, 8), :] + p_lo
        return jnp.concatenate([lo, n_hi + src[w, pl.ds(base + 7, 8), :]], axis=0)

    for w in range(NW):
        c, u, lo = splat(w)
        ctab[w, 0:1, :] = c
        if u is not None:
            ctab[w, 1:2, :] = u
        if lo is not None:
            ctab[w, 2:3, :] = lo
        if u is not None and lo is not None:
            ctab[w, 3:4, :] = OMEGA / (4.0 * c + u + lo)

    def const(w, i):
        return ctab[w, i:i + 1, :]

    def flows(src, w, y, count, above=True, below=True):
        ty, m = w % LZ, w // LZ
        xs = [src[w, rows_of(y + j), :] for j in range(-1, count + 1)]
        c = const(w, 0)
        u = const(w, 1) if ty < 3 else None
        lo = const(w, 2) if ty > 0 else None
        out = []
        for j in range(count):
            side = (xs[j] + xs[j + 2]) + beside(src, w, y + j)
            total = f[w, rows_of(y + j), :] + c * side
            if above:
                total += (vn[m + 1, rows_of(y + j), :] if ty == 3 else u) * src[w + 1, rows_of(y + j), :]
            if below:
                total += (vn[m, rows_of(y + j), :] if ty == 0 else lo) * src[w - 1, rows_of(y + j), :]
            out.append((xs[j + 1], total))
        return out

    def weight(w, y):
        ty, m = w % LZ, w // LZ
        if ty == 0:
            return wlo[m, rows_of(y), :]
        if ty == 3:
            return whi[m, rows_of(y), :]
        return const(w, 3) * fine_valid(y)

    def start_from_zero(dst, layers, y_lo, y_hi):
        def body(y):
            for w in layers:
                dst[w, rows_of(y), :] = weight(w, y) * f[w, rows_of(y), :]

        row_loop(y_lo, y_hi, max(1, 16 // len(layers)), body)

    def sweep(src, dst, layers, y_lo, y_hi):
        def body(y, count):
            for w in layers:
                for j, (x, total) in enumerate(flows(src, w, y, count)):
                    dst[w, rows_of(y + j), :] = KEEP * x + weight(w, y + j) * total

        strip_loop(y_lo, y_hi, STRIP, body)

    def diagonal(w, y):
        c = const(w, 0)
        if w == LZ:
            return 4.0 * c + const(w, 1) + vn[1, rows_of(y), :]
        if w == LZ + 3:
            return 4.0 * c + const(w, 2) + vd_top[rows_of(y), :]
        return 4.0 * c + const(w, 1) + const(w, 2)

    own_layers = list(range(LZ, 2 * LZ))

    def restricted_residual(src, slot):
        def body(i, carry):
            y = HY + i * 4
            sums = []
            for w in own_layers:
                rows = flows(src, w, y, 4, above=w < LZ + 3, below=w > LZ)
                parts = [total - diagonal(w, y + q) * x for q, (x, total) in enumerate(rows)]
                sums.append((parts[0] + parts[1]) + (parts[2] + parts[3]))
            for j, w in ((1, LZ), (2, LZ + 3)):
                parts = [vn[j, rows_of(y + q), :] * src[w, rows_of(y + q), :] for q in range(4)]
                sums.append((parts[0] + parts[1]) + (parts[2] + parts[3]))
            for s in range(4):
                restr[pl.ds(pl.multiple_of((i * 4 + s) * K, K), K), :] = sums[s]
            for s in range(2):
                restr[pl.ds(pl.multiple_of(16 * K + (i * 2 + s) * K, K), K), :] = sums[4 + s]
            return carry

        lax.fori_loop(0, 4, body, 0)
        for g, start in enumerate((0, 16 * K, 8 * K)):
            for p in range(4):
                tile = restr[pl.ds(start + 4 * p, 8, stride=K), :]
                for q in range(1, 4):
                    tile += restr[pl.ds(start + 4 * p + q, 8, stride=K), :]
                r1g[slot, d, g * 4 + p] = tile

    mid_c = 4.0 * cond
    low_c = 16.0 * cond

    def lane_next(x):
        return jnp.where(lanes16 == LANES - 1, 0.0, pltpu.roll(x, LANES - 1, 1))

    def lane_prev(x):
        return jnp.where(lanes16 == 0, 0.0, pltpu.roll(x, 1, 1))

    def mid_flows(src, rhs, i):
        xs = [src[i * 4 + p] for p in range(4)]
        out = []
        for p in range(4):
            nxt = xs[p + 1] if p < 3 else lane_next(xs[0])
            prv = xs[p - 1] if p > 0 else lane_prev(xs[3])
            side = (src[i * 4 - 4 + p] + src[i * 4 + 4 + p]) + (nxt + prv)
            total = rhs[i * 4 + p] + mid_c * side
            total += u1[i * 4 + p] * pltpu.roll(xs[p], NZ - 1, 0)
            total += l1[i * 4 + p] * pltpu.roll(xs[p], 1, 0)
            out.append((xs[p], total))
        return out

    def mid_sweep(src, dst, rhs, lo, hi):
        def body(i):
            for p, (x, total) in enumerate(mid_flows(src, rhs, i)):
                dst[i * 4 + p] = KEEP * x + w1[i * 4 + p] * total

        row_loop(lo, hi, max(u for u in (1, 2, 3, 4, 5) if (hi - lo) % u == 0), body)

    def mid_start(rhs, lo, hi):
        def body(i):
            for p in range(4):
                a1[i * 4 + p] = w1[i * 4 + p] * rhs[i * 4 + p]

        row_loop(lo, hi, 2, body)

    def assemble(slot):
        def turned(x, shift):
            return x if shift % 8 == 0 else pltpu.roll(x, shift % 8, 0)

        for i in range(4):
            half = 4 * (i % 2)
            for p in range(4):
                ts = [r1g[slot, e, (0 if i < 2 else 8) + p] for e in range(4)]
                cs = [r1g[slot, e, 4 + p] for e in range(4)]

                def put(e, down, dst_row):
                    return jnp.where(subs8 == dst_row, turned(cs[e], dst_row - (2 * i + down)), 0.0)

                lo = jnp.where(subs8 < 4, turned(ts[0], -half), turned(ts[1], 4 - half))
                lo += put(1, 0, 3) + put(0, 1, 4) + put(2, 0, 7)
                hi = jnp.where(subs8 < 4, turned(ts[2], -half), turned(ts[3], 4 - half))
                hi += put(1, 1, 0) + put(3, 0, 3) + put(2, 1, 4)
                r1[slot, (H1 + i) * 4 + p] = jnp.concatenate([lo, hi], axis=0)

    def coarse_cycle(slot, after_gather, after_spread, while_waiting):
        gather = [push(r1g.at[slot, d], r1g.at[slot, d], dd, 0) for dd in (2, 1, 3)]
        after_gather()
        arrived(gather)
        assemble(slot)
        rhs = r1.at[slot]

        def mid_rows(i, count):
            return rhs.at[pl.ds(i * 4, count * 4)]

        urgent = [
            push(mid_rows(H1 + 2, 2), mid_rows(H1 - 2, 2), 0, 1),
            push(mid_rows(H1, 2), mid_rows(H1 + 4, 2), 0, -1),
        ]
        rest = [
            push(mid_rows(H1, 2), mid_rows(H1 - 4, 2), 0, 1),
            push(mid_rows(H1 + 2, 2), mid_rows(H1 + 6, 2), 0, -1),
            push(mid_rows(H1 + 3, 1), mid_rows(0, 1), 0, 2),
            push(mid_rows(H1, 1), mid_rows(N1 - 1, 1), 0, -2),
        ]
        after_spread()
        arrived(urgent)
        mid_start(rhs, H1 - 2, H1 + 6)
        mid_sweep(a1, b1, rhs, H1 - 1, H1 + 5)

        def down(i, acc):
            for j in range(2):
                row = H1 + 2 * i + j
                for p, (x, total) in enumerate(mid_flows(b1, rhs, row)):
                    acc += total - (OMEGA / w1[row * 4 + p]) * x
            return acc

        r2[slot, H2] = lax.fori_loop(0, 2, down, jnp.zeros((NZ, LANES), F32))
        low = []
        for j in range(H2, 0, -1):
            low.append(push(r2.at[slot, H2], r2.at[slot, H2 - j], 0, j))
            low.append(push(r2.at[slot, H2], r2.at[slot, H2 + j], 0, -j))
        arrived(rest)
        mid_start(rhs, 0, H1 - 2)
        mid_start(rhs, H1 + 6, N1)
        mid_sweep(a1, b1, rhs, 1, H1 - 1)
        mid_sweep(a1, b1, rhs, H1 + 5, N1 - 1)
        while_waiting()
        arrived(low)

        bufs = (a2, b2)
        for i in range(N2):
            a2[i] = w2[i] * r2[slot, i]
        for s in range(5):
            src, dst = bufs[s % 2], bufs[(s + 1) % 2]
            for i in range(s + 1, N2 - 1 - s):
                x = src[i]
                side = (src[i - 1] + src[i + 1]) + (lane_next(x) + lane_prev(x))
                total = r2[slot, i] + low_c * side
                total += u2[i] * pltpu.roll(x, NZ - 1, 0) + l2[i] * pltpu.roll(x, 1, 0)
                dst[i] = KEEP * x + w2[i] * total
        fix = bufs[1]
        for g in range(3):
            e2 = fix[H2 - 1 + g]
            for i in range(4):
                for p in range(4):
                    at_cell = (H1 - 4 + g * 4 + i) * 4 + p
                    b1[at_cell] = b1[at_cell] + e2
        mid_sweep(b1, a1, rhs, 2, N1 - 2)
        mid_sweep(a1, b1, rhs, 3, N1 - 3)
        sent(gather + urgent + rest + low)

    def correction(i, w):
        z = lax.rem(LZ * (d + 3) + w, NZ)
        rows = [b1[i * 4 + p, pl.ds(z, 1), :] for p in range(4)]
        lo = jnp.where(subs8 < 4, rows[0], rows[1])
        hi = jnp.where(subs8 < 4, rows[2], rows[3])
        return jnp.concatenate([lo, hi], axis=0)

    def correct(layers, i_lo, i_hi, edge_rows, pick, dst):
        def row(i, y, fix, w):
            dst[w, rows_of(y), :] = pick(w, y) * fine_valid(y) + fix

        def body(i):
            for w in layers:
                fix = correction(i, w)
                for q in range(4):
                    row(i, HY + (i - H1) * 4 + q, fix, w)

        row_loop(i_lo, i_hi, 1, body)
        for y in edge_rows:
            i = (y - HY) // 4 + H1
            for w in layers:
                row(i, y, correction(i, w), w)

    arrived(near[2:4])
    start_from_zero(v0, own_layers, HY - 2, HY + ROWS + 2)
    sweep(v0, v1, [5, 6], HY - 1, HY + ROWS + 1)
    arrived(near[0:2] + near[4:])
    start_from_zero(v0, [3, 8], HY - 1, HY + ROWS + 1)
    sweep(v0, v1, [4, 7], HY - 1, HY + ROWS + 1)
    restricted_residual(v1, 0)

    later = []
    forwarded = []
    far_source = []
    all_layers = list(range(NW))
    inner = list(range(1, NW - 1))

    def background_one():
        far_source.extend([
            push(f.at[5, rows_of(HY + 8, 8)], f.at[1, rows_of(HY + 8, 8)], 1, 0),
            push(f.at[6, rows_of(HY + 8, 8)], f.at[10, rows_of(HY + 8, 8)], -1, 0),
        ])
        later.extend([
            push(v1.at[pl.ds(4, 2), own], v1.at[pl.ds(0, 2), own], 1, 0),
            push(v1.at[pl.ds(6, 2), own], v1.at[pl.ds(10, 2), own], -1, 0),
            push(v1.at[pl.ds(4, 2), rows_of(last - 1, 2)], v1.at[pl.ds(0, 2), rows_of(HY - 2, 2)], 1, 1),
            push(v1.at[pl.ds(4, 2), rows_of(HY, 2)], v1.at[pl.ds(0, 2), rows_of(last + 1, 2)], 1, -1),
            push(v1.at[pl.ds(6, 2), rows_of(last - 1, 2)], v1.at[pl.ds(10, 2), rows_of(HY - 2, 2)], -1, 1),
            push(v1.at[pl.ds(6, 2), rows_of(HY, 2)], v1.at[pl.ds(10, 2), rows_of(last + 1, 2)], -1, -1),
        ])
        remaining_coefficients()
        arrived(bulk)
        forward(1)
        forward(2)

    def forward(far):
        count = HY - far if far > 1 else HY - 2
        low_row, high_row = far, last + 1 + (1 if far == 1 else 0)
        for w in (LZ - far, 2 * LZ - 1 + far):
            forwarded.append(push(f.at[w, rows_of(low_row + ROWS, count)], f.at[w, rows_of(low_row, count)], 0, 1))
            forwarded.append(push(f.at[w, rows_of(high_row - ROWS, count)], f.at[w, rows_of(high_row, count)], 0, -1))

    outer = [2, 3, 8, 9]

    def forward_last():
        arrived(far_source)
        forward(3)

    def window_inside():
        start_from_zero(v0, [1, 2, 3, 8, 9, 10], HY, HY + ROWS)
        sweep(v0, v1, outer, HY + 1, HY + ROWS - 1)

    def presmooth_window():
        window_inside()
        arrived(forwarded)
        sent(later)
        for lo, hi in ((0, HY), (HY + ROWS, NYW)):
            start_from_zero(v0, inner, lo, hi)
        sweep(v0, v1, own_layers, 1, HY - 1)
        sweep(v0, v1, own_layers, HY + ROWS + 1, NYW - 1)
        sweep(v0, v1, outer, 1, HY + 1)
        sweep(v0, v1, outer, HY + ROWS - 1, NYW - 1)

    coarse_cycle(0, background_one, forward_last, presmooth_window)
    arrived(later)
    correct(all_layers, H1 - 1, H1 + 5, (1, NYW - 2), lambda w, y: v1[w, rows_of(y), :], v1)
    bufs = (v1, v0)
    for s in range(4):
        sweep(bufs[s % 2], bufs[(s + 1) % 2], list(range(s + 1, NW - 1 - s)), s + 2, NYW - 2 - s)
    restricted_residual(v1, 1)

    tail = []

    def background_two():
        tail.extend([
            push(v1.at[pl.ds(5, 3), own], v2.at[pl.ds(1, 3), own], 1, 0),
            push(v1.at[pl.ds(4, 3), own], v2.at[pl.ds(8, 3), own], -1, 0),
            push(v1.at[pl.ds(4, 4), rows_of(last - 2, 3)], v2.at[pl.ds(4, 4), rows_of(HY - 3, 3)], 0, 1),
            push(v1.at[pl.ds(4, 4), rows_of(HY, 3)], v2.at[pl.ds(4, 4), rows_of(last + 1, 3)], 0, -1),
            push(v1.at[pl.ds(6, 2), rows_of(last - 1, 2)], v2.at[pl.ds(2, 2), rows_of(HY - 2, 2)], 1, 1),
            push(v1.at[pl.ds(6, 2), rows_of(HY, 2)], v2.at[pl.ds(2, 2), rows_of(last + 1, 2)], 1, -1),
            push(v1.at[pl.ds(4, 2), rows_of(last - 1, 2)], v2.at[pl.ds(8, 2), rows_of(HY - 2, 2)], -1, 1),
            push(v1.at[pl.ds(4, 2), rows_of(HY, 2)], v2.at[pl.ds(8, 2), rows_of(last + 1, 2)], -1, -1),
        ])

    coarse_cycle(1, background_two, lambda: None, lambda: None)
    arrived(tail)

    def keep_own(y):
        for w in own_layers:
            v2[w, rows_of(y), :] = v1[w, rows_of(y), :]

    row_loop(HY, HY + ROWS, 4, keep_own)
    deep = list(range(1, NW - 1))
    correct(deep, H1 - 1, H1 + 5, (), lambda w, y: v2[w, rows_of(y), :], v0)
    sent(tail)
    sweep(v0, v1, deep[1:-1], HY - 2, HY + ROWS + 2)
    sweep(v1, v0, deep[2:-2], HY - 1, HY + ROWS + 1)

    def defect(y, count):
        for w in own_layers:
            for j, (x, total) in enumerate(flows(v0, w, y, count)):
                v2[w, rows_of(y + j), :] = total - diagonal(w, y + j) * x

    strip_loop(HY, HY + ROWS, 4, defect)

    for k in range(K):
        block = jnp.concatenate([src[w, pl.ds(HY * K + k, ROWS, stride=K), :]
                                 for src in (v0, v2) for w in own_layers], axis=0)
        out[pl.ds(k, LANES, stride=K), :] = block.T
    sent(par + near + bulk + far_source + forwarded)


OUT_PARTS = 4


def natural(turned_in, v_out, b_out, turned, v_vm, b_vm, sem):
    copies = []
    per = K // OUT_PARTS
    loads = []
    for g in range(OUT_PARTS):
        part = pl.ds(g * per * LANES, per * LANES)
        loads.append(pltpu.make_async_copy(turned_in.at[part], turned.at[part], sem.at[2, g]))
        loads[g].start()
    for g in range(OUT_PARTS):
        loads[g].wait()
        for m in range(g * per, (g + 1) * per):
            block = turned[m * LANES:(m + 1) * LANES, :].T
            v_vm[:, :, m * LANES:(m + 1) * LANES] = block[0:LZ * ROWS].reshape(LZ, ROWS, LANES)
            b_vm[:, :, m * LANES:(m + 1) * LANES] = block[LZ * ROWS:].reshape(LZ, ROWS, LANES)
        part = (slice(None), slice(None), pl.ds(g * per * LANES, per * LANES))
        for i, (src, dst) in enumerate(((v_vm, v_out), (b_vm, b_out))):
            copies.append(pltpu.make_async_copy(src.at[part], dst.at[part], sem.at[i, g]))
            copies[-1].start()
    for copy in copies:
        copy.wait()


N_COPIES = 3 + 8 + 4 + 8 + 12 + 8 + 2 * (3 + 6 + 2 * H2)


def local(n_tile, source_heating, material_thermal_values, layer_material, via_conductance, via_blocks):
    def tiles(*lead):
        return pltpu.VMEM(lead + (NZ, LANES), F32)

    def window(n):
        return pltpu.VMEM((n, NYW * K, LANES), F32)

    vmem = pl.BlockSpec(memory_space=pltpu.VMEM)
    shape = jax.ShapeDtypeStruct(source_heating.shape, F32)
    turned = pl.pallas_call(
        functools.partial(kernel, n_tile),
        out_shape=jax.ShapeDtypeStruct((K * LANES, LANES), F32),
        in_specs=[pl.BlockSpec(memory_space=pltpu.HBM)] * 5,
        out_specs=vmem,
        scratch_shapes=[
            pltpu.SMEM(material_thermal_values.shape, F32), pltpu.SMEM(layer_material.shape, jnp.int32),
            pltpu.SMEM(via_conductance.shape, F32), pltpu.VMEM((1, 4, via_blocks.shape[1]), jnp.int32),
            pltpu.VMEM(source_heating.shape, F32),
            window(NW), window(NW), window(NW), window(NW), window(4),
            pltpu.VMEM((NYW * K, LANES), F32), window(3), window(3),
            pltpu.VMEM((4, 8, LANES), F32), tiles(2),
            pltpu.VMEM((K * LANES, LANES), F32), pltpu.VMEM((4 * 6 * K, LANES), F32),
            pltpu.VMEM((2, 4, 12, 8, LANES), F32), tiles(2, N1 * 4),
            tiles(N1 * 4), tiles(N1 * 4), tiles(N1 * 4), tiles(N1 * 4), tiles(N1 * 4),
            tiles(2, N2), tiles(N2), tiles(N2), tiles(N2), tiles(N2), tiles(N2),
            pltpu.VMEM((4, 80, LANES), F32), pltpu.VMEM((8, LANES), F32),
            pltpu.VMEM((NW, 8, LANES), F32),
            pltpu.SemaphoreType.DMA((N_COPIES,)),
            pltpu.SemaphoreType.DMA((N_COPIES,)),
            pltpu.SemaphoreType.DMA((8,)),
        ],
        compiler_params=pltpu.CompilerParams(collective_id=0, has_side_effects=True),
    )(source_heating, material_thermal_values, layer_material, via_conductance, via_blocks.transpose(0, 2, 1))
    anywhere = pl.BlockSpec(memory_space=pl.ANY)
    return pl.pallas_call(
        natural,
        out_shape=(shape, shape),
        in_specs=[anywhere],
        out_specs=(anywhere, anywhere),
        scratch_shapes=[pltpu.VMEM((K * LANES, LANES), F32), pltpu.VMEM(source_heating.shape, F32), pltpu.VMEM(source_heating.shape, F32),
                        pltpu.SemaphoreType.DMA((3, OUT_PARTS))],
    )(turned)


def solution(mesh):
    in_specs = (P("die", "tile", None), P(), P("die"), P("die"), P("die", None, None))
    out_specs = (P("die", "tile", None), P("die", "tile", None))
    body = functools.partial(local, mesh.shape["tile"])
    return jax.shard_map(body, mesh=mesh, in_specs=in_specs, out_specs=out_specs, check_vma=False)
```

```python
import functools

import jax
import jax.numpy as jnp
from jax import lax
from jax.experimental import pallas as pl
from jax.experimental.pallas import tpu as pltpu
from jax.sharding import PartitionSpec as P

F32 = jnp.float32
OMEGA = 0.8
KEEP = 1.0 - OMEGA
LZ = 4
ROWS = 16
HY = 6
NYW = ROWS + 2 * HY
NW = 3 * LZ
K = 16
LANES = 128
H1 = 5
N1 = 4 + 2 * H1
H2 = 6
N2 = 1 + 2 * H2
NZ = 16
STRIP = 12


def rows_of(y, count=1):
    start = y * K
    if not isinstance(start, int):
        start = pl.multiple_of(start, K)
    return pl.ds(start, count * K)


def row_loop(lo, hi, unroll, fn):
    whole = (hi - lo) // unroll

    def body(i, carry):
        for j in range(unroll):
            fn(lo + i * unroll + j)
        return carry

    if whole:
        lax.fori_loop(0, whole, body, 0)
    for y in range(lo + whole * unroll, hi):
        fn(y)


def strip_loop(lo, hi, unroll, fn):
    whole = (hi - lo) // unroll

    def body(i, carry):
        fn(lo + i * unroll, unroll)
        return carry

    if whole:
        lax.fori_loop(0, whole, body, 0)
    if lo + whole * unroll < hi:
        fn(lo + whole * unroll, hi - lo - whole * unroll)


def kernel(n_tile, f_in, mats_in, material_in, via_cond_in, blocks_in, out, mats, material, via_cond, blocks, f_vm, f, v0, v1, v2, vn, vd_top, wlo, whi, pall, cz,
           turn, restr, r1g, r1, w1, u1, l1, a1, b1, r2, w2, u2, l2, a2, b2, via1, pk, ctab, send_sem, recv_sem, in_sem):
    d = lax.axis_index("die")
    t = lax.axis_index("tile")

    def at(dd, dt):
        return {"die": lax.rem(d + dd + 4, 4), "tile": lax.rem(t + dt + n_tile, n_tile)}

    counter = [0]

    def push(src, dst, dd, dt):
        i = counter[0]
        counter[0] += 1
        copy = pltpu.make_async_remote_copy(
            src_ref=src, dst_ref=dst, send_sem=send_sem.at[i], recv_sem=recv_sem.at[i],
            device_id=at(dd, dt), device_id_type=pl.DeviceIdType.MESH)
        copy.start()
        return copy

    def arrived(copies):
        for copy in copies:
            copy.wait_recv()

    def sent(copies):
        for copy in copies:
            copy.wait_send()

    loads = []
    for g in range(4):
        part = (slice(None), slice(None), pl.ds(g * 4 * LANES, 4 * LANES))
        loads.append(pltpu.make_async_copy(f_in.at[part], f_vm.at[part], in_sem.at[g]))
        loads[g].start()

    small = []
    for g, (src, dst) in enumerate(((mats_in, mats), (material_in, material), (via_cond_in, via_cond), (blocks_in, blocks))):
        small.append(pltpu.make_async_copy(src, dst, in_sem.at[4 + g]))
        small[g].start()

    partners = [(1, 0), (2, 0), (3, 0), (1, 1), (1, -1), (-1, 1), (-1, -1)]
    partners += [(0, s * j) for j in range(1, 5) for s in (1, -1)]
    barrier = pltpu.get_barrier_semaphore()
    for dd, dt in partners:
        pl.semaphore_signal(barrier, inc=1, device_id=at(dd, dt), device_id_type=pl.DeviceIdType.MESH)

    for g in range(4):
        loads[g].wait()
        for m in range(4 * g, 4 * g + 4):
            block = f_vm[:, :, m * LANES:(m + 1) * LANES].reshape(LZ * ROWS, LANES)
            turn[m * LANES:(m + 1) * LANES, 0:LZ * ROWS] = block.T
    for k in range(K):
        block = turn[pl.ds(k, LANES, stride=K), 0:LZ * ROWS].T
        for z in range(LZ):
            f[LZ + z, pl.ds(HY * K + k, ROWS, stride=K), :] = block[z * ROWS:(z + 1) * ROWS]
    zero_row = jnp.zeros((K, LANES), F32)

    def clear(y):
        for w in (0, 1, NW - 2, NW - 1):
            v1[w, rows_of(y), :] = zero_row

    row_loop(0, NYW, 4, clear)

    for copy in small:
        copy.wait()
    pk[0:4, :] = jnp.full((4, LANES), via_cond[0], F32)
    pk[0:4, 0:24] = blocks[0].astype(F32)
    for z in range(LZ):
        pk[4 + z:5 + z, :] = jnp.full((1, LANES), mats[material[z]], F32)
    pall[d] = pk[...]

    def coverage(e, rows, row0, cell, lanes_cols):
        n_lanes = lanes_cols * LANES
        prm = pall[e]
        down = prm.T
        lane = lax.broadcasted_iota(jnp.int32, (24, n_lanes), 1)
        col = (((lane & (LANES - 1)) * lanes_cols + (lane >> 7)) * cell).astype(F32)
        c_lo, c_hi = down[0:24, 1:2], down[0:24, 1:2] + down[0:24, 3:4]
        cols = jnp.maximum(jnp.minimum(c_hi, col + cell) - jnp.maximum(c_lo, col), 0.0)
        row = ((row0 + lax.broadcasted_iota(jnp.int32, (rows, LANES), 0)) * cell).astype(F32)
        r_lo, r_hi = prm[0:1, :], prm[0:1, :] + prm[2:3, :]
        cover = jnp.maximum(jnp.minimum(r_hi, row + cell) - jnp.maximum(r_lo, row), 0.0)
        return jnp.dot(cover[:, 0:24], cols, precision=lax.Precision.HIGHEST,
                       preferred_element_type=F32) * prm[0:1, LANES - 1:]

    zs = lax.broadcasted_iota(jnp.int32, (NZ, LANES), 0)
    is_top = (zs & 3) == 3
    is_end = zs == NZ - 1
    lanes8 = lax.broadcasted_iota(jnp.int32, (8, LANES), 1)
    subs8 = lax.broadcasted_iota(jnp.int32, (8, LANES), 0)
    lanes16 = lax.broadcasted_iota(jnp.int32, (NZ, LANES), 1)

    def valid(row, count):
        return jnp.where((row >= 0) & (row < count), 1.0, 0.0).astype(F32)

    def fine_valid(y):
        return valid(t * ROWS - HY + y, n_tile * ROWS)

    def via_plane(j):
        plane = coverage(lax.rem(d + 2 + j, 4), 32, t * ROWS - HY, 1, K)
        for k in range(K):
            vn[j, pl.ds(k, NYW, stride=K), :] = plane[0:NYW, k * LANES:(k + 1) * LANES]

    pl.semaphore_wait(barrier, len(partners))

    own = rows_of(HY, ROWS)
    last = HY + ROWS - 1
    par = [push(pk, pall.at[d], dd, 0) for dd in (1, 2, 3)]
    near = [
        push(f.at[7, own], f.at[3, own], 1, 0),
        push(f.at[4, own], f.at[8, own], -1, 0),
        push(f.at[pl.ds(4, 4), rows_of(last + 1 - HY, HY)], f.at[pl.ds(4, 4), rows_of(0, HY)], 0, 1),
        push(f.at[pl.ds(4, 4), rows_of(HY, HY)], f.at[pl.ds(4, 4), rows_of(HY + ROWS, HY)], 0, -1),
        push(f.at[7, rows_of(last)], f.at[3, rows_of(HY - 1)], 1, 1),
        push(f.at[7, rows_of(HY)], f.at[3, rows_of(last + 1)], 1, -1),
        push(f.at[4, rows_of(last)], f.at[8, rows_of(HY - 1)], -1, 1),
        push(f.at[4, rows_of(HY)], f.at[8, rows_of(last + 1)], -1, -1),
    ]
    bulk = [
        push(f.at[6, own], f.at[2, own], 1, 0),
        push(f.at[5, own], f.at[9, own], -1, 0),
        push(f.at[5, rows_of(HY, 8)], f.at[1, rows_of(HY, 8)], 1, 0),
        push(f.at[6, rows_of(HY, 8)], f.at[10, rows_of(HY, 8)], -1, 0),
    ]

    def clear_v2(y):
        for w in range(NW):
            v2[w, rows_of(y), :] = zero_row

    row_loop(0, NYW, 2, clear_v2)
    via_plane(2)
    arrived(par)
    via_plane(1)

    cond = jnp.concatenate([pall[e, 4:8, :] for e in range(4)], axis=0)
    follow = jnp.concatenate([cond[1:], cond[NZ - 1:]], axis=0)
    vert = 2.0 * cond * follow / (cond + follow)
    cz[0] = cond
    cz[1] = vert

    def zrow(which, w):
        z = lax.rem(LZ * (d + 3) + w, NZ)
        return cz[which, pl.ds(z, 1), :]

    def splat(w):
        ty = w % LZ
        c = zrow(0, w)
        u = zrow(1, w) if ty < 3 else None
        lo = zrow(1, w - 1) if ty > 0 else None
        return c, u, lo

    edge = [jnp.where(lax.rem(d + 2 + j, 4) == 3, 0.0, 1.0).astype(F32) for j in range(4)]
    ends = [(splat(LZ * m), splat(LZ * m + 3)) for m in range(3)]

    def weight_below(m, y, ok, coupled):
        c, u, _ = ends[m][0]
        wlo[m, rows_of(y), :] = ok / (4.0 * c + u + coupled)

    def weight_above(m, y, ok, plane):
        c, _, lo = ends[m][1]
        whi[m, rows_of(y), :] = ok / (4.0 * c + lo + plane)

    def near_weights(y):
        ok = fine_valid(y) * OMEGA
        planes = {j: vn[j, rows_of(y), :] for j in (1, 2)}
        vd_top[rows_of(y), :] = planes[2]
        for j in (1, 2):
            coupled = planes[j] * edge[j]
            vn[j, rows_of(y), :] = coupled
            weight_below(j, y, ok, coupled)
            weight_above(j - 1, y, ok, planes[j])

    row_loop(0, NYW, 4, near_weights)

    def far_weights(y):
        ok = fine_valid(y) * OMEGA
        planes = {j: vn[j, rows_of(y), :] for j in (0, 3)}
        for j in (0, 3):
            vn[j, rows_of(y), :] = planes[j] * edge[j]
        weight_below(0, y, ok, planes[0] * edge[0])
        weight_above(2, y, ok, planes[3])

    def coarse_coeffs(via_rows, scale, couple, row_ok):
        via = jnp.zeros((NZ, LANES), F32)
        for e in range(4):
            via = jnp.where(zs == LZ * e + 3, via_rows[e], via)
        upper = jnp.where(is_top, via, vert * couple)
        nb = jnp.where(is_end, 0.0, upper)
        lower = pltpu.roll(nb, 1, 0)
        return (row_ok * OMEGA) / (4.0 * scale * cond + upper + lower), nb, lower

    def mid_coeffs(i):
        ok = valid(t * 4 - H1 + i, n_tile * 4)
        for p in range(4):
            got = coarse_coeffs([via1[e, pl.ds(p * 16 + i, 1), :] for e in range(4)], 4.0, 16.0, ok)
            w1[i * 4 + p], u1[i * 4 + p], l1[i * 4 + p] = got

    def low_coeffs(i):
        ok = valid(t - H2 + i, n_tile)
        got = coarse_coeffs([via1[e, pl.ds(64 + i, 1), :] for e in range(4)], 16.0, 256.0, ok)
        w2[i], u2[i], l2[i] = got

    def remaining_coefficients():
        for e in range(4):
            plane = coverage(e, 16, t * 4 - H1, 4, 4)
            for p in range(4):
                via1[e, p * 16:(p + 1) * 16, :] = plane[:, p * LANES:(p + 1) * LANES]
            via1[e, 64:80, :] = coverage(e, 16, t - H2, 16, 1)
        row_loop(0, N1, 2, mid_coeffs)
        row_loop(0, N2, 4, low_coeffs)
        via_plane(0)
        via_plane(3)
        row_loop(0, NYW, 4, far_weights)

    def beside(src, w, y):
        base = y * K if isinstance(y, int) else pl.multiple_of(y * K, K)
        first = jnp.broadcast_to(src[w, pl.ds(base, 1), :], (8, LANES))
        final = jnp.broadcast_to(src[w, pl.ds(base + K - 1, 1), :], (8, LANES))
        n_in = jnp.where(lanes8 == LANES - 1, 0.0, pltpu.roll(first, LANES - 1, 1))
        p_in = jnp.where(lanes8 == 0, 0.0, pltpu.roll(final, 1, 1))
        n_hi = jnp.where(subs8 == 7, n_in, src[w, pl.ds(base + 9, 8), :])
        p_lo = jnp.where(subs8 == 0, p_in, src[w, pl.ds(base - 1, 8), :])
        lo = src[w, pl.ds(base + 1, 8), :] + p_lo
        return jnp.concatenate([lo, n_hi + src[w, pl.ds(base + 7, 8), :]], axis=0)

    for w in range(NW):
        c, u, lo = splat(w)
        ctab[w, 0:1, :] = c
        if u is not None:
            ctab[w, 1:2, :] = u
        if lo is not None:
            ctab[w, 2:3, :] = lo
        if u is not None and lo is not None:
            ctab[w, 3:4, :] = OMEGA / (4.0 * c + u + lo)

    def const(w, i):
        return ctab[w, i:i + 1, :]

    def flows(src, w, y, count, above=True, below=True):
        ty, m = w % LZ, w // LZ
        xs = [src[w, rows_of(y + j), :] for j in range(-1, count + 1)]
        c = const(w, 0)
        u = const(w, 1) if ty < 3 else None
        lo = const(w, 2) if ty > 0 else None
        out = []
        for j in range(count):
            side = (xs[j] + xs[j + 2]) + beside(src, w, y + j)
            total = f[w, rows_of(y + j), :] + c * side
            if above:
                total += (vn[m + 1, rows_of(y + j), :] if ty == 3 else u) * src[w + 1, rows_of(y + j), :]
            if below:
                total += (vn[m, rows_of(y + j), :] if ty == 0 else lo) * src[w - 1, rows_of(y + j), :]
            out.append((xs[j + 1], total))
        return out

    def weight(w, y):
        ty, m = w % LZ, w // LZ
        if ty == 0:
            return wlo[m, rows_of(y), :]
        if ty == 3:
            return whi[m, rows_of(y), :]
        return const(w, 3) * fine_valid(y)

    def start_from_zero(dst, layers, y_lo, y_hi):
        def body(y):
            for w in layers:
                dst[w, rows_of(y), :] = weight(w, y) * f[w, rows_of(y), :]

        row_loop(y_lo, y_hi, max(1, 16 // len(layers)), body)

    def sweep(src, dst, layers, y_lo, y_hi):
        def body(y, count):
            for w in layers:
                for j, (x, total) in enumerate(flows(src, w, y, count)):
                    dst[w, rows_of(y + j), :] = KEEP * x + weight(w, y + j) * total

        strip_loop(y_lo, y_hi, STRIP, body)

    def diagonal(w, y):
        c = const(w, 0)
        if w == LZ:
            return 4.0 * c + const(w, 1) + vn[1, rows_of(y), :]
        if w == LZ + 3:
            return 4.0 * c + const(w, 2) + vd_top[rows_of(y), :]
        return 4.0 * c + const(w, 1) + const(w, 2)

    own_layers = list(range(LZ, 2 * LZ))

    def restricted_residual(src, slot):
        def body(i, carry):
            y = HY + i * 4
            sums = []
            for w in own_layers:
                rows = flows(src, w, y, 4, above=w < LZ + 3, below=w > LZ)
                parts = [total - diagonal(w, y + q) * x for q, (x, total) in enumerate(rows)]
                sums.append((parts[0] + parts[1]) + (parts[2] + parts[3]))
            for j, w in ((1, LZ), (2, LZ + 3)):
                parts = [vn[j, rows_of(y + q), :] * src[w, rows_of(y + q), :] for q in range(4)]
                sums.append((parts[0] + parts[1]) + (parts[2] + parts[3]))
            for s in range(4):
                restr[pl.ds(pl.multiple_of((i * 4 + s) * K, K), K), :] = sums[s]
            for s in range(2):
                restr[pl.ds(pl.multiple_of(16 * K + (i * 2 + s) * K, K), K), :] = sums[4 + s]
            return carry

        lax.fori_loop(0, 4, body, 0)
        for g, start in enumerate((0, 16 * K, 8 * K)):
            for p in range(4):
                tile = restr[pl.ds(start + 4 * p, 8, stride=K), :]
                for q in range(1, 4):
                    tile += restr[pl.ds(start + 4 * p + q, 8, stride=K), :]
                r1g[slot, d, g * 4 + p] = tile

    mid_c = 4.0 * cond
    low_c = 16.0 * cond

    def lane_next(x):
        return jnp.where(lanes16 == LANES - 1, 0.0, pltpu.roll(x, LANES - 1, 1))

    def lane_prev(x):
        return jnp.where(lanes16 == 0, 0.0, pltpu.roll(x, 1, 1))

    def mid_flows(src, rhs, i):
        xs = [src[i * 4 + p] for p in range(4)]
        out = []
        for p in range(4):
            nxt = xs[p + 1] if p < 3 else lane_next(xs[0])
            prv = xs[p - 1] if p > 0 else lane_prev(xs[3])
            side = (src[i * 4 - 4 + p] + src[i * 4 + 4 + p]) + (nxt + prv)
            total = rhs[i * 4 + p] + mid_c * side
            total += u1[i * 4 + p] * pltpu.roll(xs[p], NZ - 1, 0)
            total += l1[i * 4 + p] * pltpu.roll(xs[p], 1, 0)
            out.append((xs[p], total))
        return out

    def mid_sweep(src, dst, rhs, lo, hi):
        def body(i):
            for p, (x, total) in enumerate(mid_flows(src, rhs, i)):
                dst[i * 4 + p] = KEEP * x + w1[i * 4 + p] * total

        row_loop(lo, hi, max(u for u in (1, 2, 3, 4, 5) if (hi - lo) % u == 0), body)

    def mid_start(rhs, lo, hi):
        def body(i):
            for p in range(4):
                a1[i * 4 + p] = w1[i * 4 + p] * rhs[i * 4 + p]

        row_loop(lo, hi, 2, body)

    def assemble(slot):
        def turned(x, shift):
            return x if shift % 8 == 0 else pltpu.roll(x, shift % 8, 0)

        for i in range(4):
            half = 4 * (i % 2)
            for p in range(4):
                ts = [r1g[slot, e, (0 if i < 2 else 8) + p] for e in range(4)]
                cs = [r1g[slot, e, 4 + p] for e in range(4)]

                def put(e, down, dst_row):
                    return jnp.where(subs8 == dst_row, turned(cs[e], dst_row - (2 * i + down)), 0.0)

                lo = jnp.where(subs8 < 4, turned(ts[0], -half), turned(ts[1], 4 - half))
                lo += put(1, 0, 3) + put(0, 1, 4) + put(2, 0, 7)
                hi = jnp.where(subs8 < 4, turned(ts[2], -half), turned(ts[3], 4 - half))
                hi += put(1, 1, 0) + put(3, 0, 3) + put(2, 1, 4)
                r1[slot, (H1 + i) * 4 + p] = jnp.concatenate([lo, hi], axis=0)

    def coarse_cycle(slot, after_gather, after_spread, while_waiting):
        gather = [push(r1g.at[slot, d], r1g.at[slot, d], dd, 0) for dd in (2, 1, 3)]
        after_gather()
        arrived(gather)
        assemble(slot)
        rhs = r1.at[slot]

        def mid_rows(i, count):
            return rhs.at[pl.ds(i * 4, count * 4)]

        urgent = [
            push(mid_rows(H1 + 2, 2), mid_rows(H1 - 2, 2), 0, 1),
            push(mid_rows(H1, 2), mid_rows(H1 + 4, 2), 0, -1),
        ]
        rest = [
            push(mid_rows(H1, 2), mid_rows(H1 - 4, 2), 0, 1),
            push(mid_rows(H1 + 2, 2), mid_rows(H1 + 6, 2), 0, -1),
            push(mid_rows(H1 + 3, 1), mid_rows(0, 1), 0, 2),
            push(mid_rows(H1, 1), mid_rows(N1 - 1, 1), 0, -2),
        ]
        after_spread()
        arrived(urgent)
        mid_start(rhs, H1 - 2, H1 + 6)
        mid_sweep(a1, b1, rhs, H1 - 1, H1 + 5)

        def down(i, acc):
            for j in range(2):
                row = H1 + 2 * i + j
                for p, (x, total) in enumerate(mid_flows(b1, rhs, row)):
                    acc += total - (OMEGA / w1[row * 4 + p]) * x
            return acc

        r2[slot, H2] = lax.fori_loop(0, 2, down, jnp.zeros((NZ, LANES), F32))
        low = []
        for j in range(H2, 0, -1):
            low.append(push(r2.at[slot, H2], r2.at[slot, H2 - j], 0, j))
            low.append(push(r2.at[slot, H2], r2.at[slot, H2 + j], 0, -j))
        arrived(rest)
        mid_start(rhs, 0, H1 - 2)
        mid_start(rhs, H1 + 6, N1)
        mid_sweep(a1, b1, rhs, 1, H1 - 1)
        mid_sweep(a1, b1, rhs, H1 + 5, N1 - 1)
        while_waiting()
        arrived(low)

        bufs = (a2, b2)
        for i in range(N2):
            a2[i] = w2[i] * r2[slot, i]
        for s in range(5):
            src, dst = bufs[s % 2], bufs[(s + 1) % 2]
            for i in range(s + 1, N2 - 1 - s):
                x = src[i]
                side = (src[i - 1] + src[i + 1]) + (lane_next(x) + lane_prev(x))
                total = r2[slot, i] + low_c * side
                total += u2[i] * pltpu.roll(x, NZ - 1, 0) + l2[i] * pltpu.roll(x, 1, 0)
                dst[i] = KEEP * x + w2[i] * total
        fix = bufs[1]
        for g in range(3):
            e2 = fix[H2 - 1 + g]
            for i in range(4):
                for p in range(4):
                    at_cell = (H1 - 4 + g * 4 + i) * 4 + p
                    b1[at_cell] = b1[at_cell] + e2
        mid_sweep(b1, a1, rhs, 2, N1 - 2)
        mid_sweep(a1, b1, rhs, 3, N1 - 3)
        sent(gather + urgent + rest + low)

    def correction(i, w):
        z = lax.rem(LZ * (d + 3) + w, NZ)
        rows = [b1[i * 4 + p, pl.ds(z, 1), :] for p in range(4)]
        lo = jnp.where(subs8 < 4, rows[0], rows[1])
        hi = jnp.where(subs8 < 4, rows[2], rows[3])
        return jnp.concatenate([lo, hi], axis=0)

    def correct(layers, i_lo, i_hi, edge_rows, pick, dst):
        def row(i, y, fix, w):
            dst[w, rows_of(y), :] = pick(w, y) * fine_valid(y) + fix

        def body(i):
            for w in layers:
                fix = correction(i, w)
                for q in range(4):
                    row(i, HY + (i - H1) * 4 + q, fix, w)

        row_loop(i_lo, i_hi, 1, body)
        for y in edge_rows:
            i = (y - HY) // 4 + H1
            for w in layers:
                row(i, y, correction(i, w), w)

    arrived(near[2:4])
    start_from_zero(v0, own_layers, HY - 2, HY + ROWS + 2)
    sweep(v0, v1, [5, 6], HY - 1, HY + ROWS + 1)
    arrived(near[0:2] + near[4:])
    start_from_zero(v0, [3, 8], HY - 1, HY + ROWS + 1)
    sweep(v0, v1, [4, 7], HY - 1, HY + ROWS + 1)
    restricted_residual(v1, 0)

    later = []
    forwarded = []
    far_source = []
    all_layers = list(range(NW))
    inner = list(range(1, NW - 1))

    def background_one():
        far_source.extend([
            push(f.at[5, rows_of(HY + 8, 8)], f.at[1, rows_of(HY + 8, 8)], 1, 0),
            push(f.at[6, rows_of(HY + 8, 8)], f.at[10, rows_of(HY + 8, 8)], -1, 0),
        ])
        later.extend([
            push(v1.at[pl.ds(4, 2), own], v1.at[pl.ds(0, 2), own], 1, 0),
            push(v1.at[pl.ds(6, 2), own], v1.at[pl.ds(10, 2), own], -1, 0),
            push(v1.at[pl.ds(4, 2), rows_of(last - 1, 2)], v1.at[pl.ds(0, 2), rows_of(HY - 2, 2)], 1, 1),
            push(v1.at[pl.ds(4, 2), rows_of(HY, 2)], v1.at[pl.ds(0, 2), rows_of(last + 1, 2)], 1, -1),
            push(v1.at[pl.ds(6, 2), rows_of(last - 1, 2)], v1.at[pl.ds(10, 2), rows_of(HY - 2, 2)], -1, 1),
            push(v1.at[pl.ds(6, 2), rows_of(HY, 2)], v1.at[pl.ds(10, 2), rows_of(last + 1, 2)], -1, -1),
        ])
        remaining_coefficients()
        arrived(bulk)
        forward(1)
        forward(2)

    def forward(far):
        count = HY - far if far > 1 else HY - 2
        low_row, high_row = far, last + 1 + (1 if far == 1 else 0)
        for w in (LZ - far, 2 * LZ - 1 + far):
            forwarded.append(push(f.at[w, rows_of(low_row + ROWS, count)], f.at[w, rows_of(low_row, count)], 0, 1))
            forwarded.append(push(f.at[w, rows_of(high_row - ROWS, count)], f.at[w, rows_of(high_row, count)], 0, -1))

    outer = [2, 3, 8, 9]

    def forward_last():
        arrived(far_source)
        forward(3)

    def window_inside():
        start_from_zero(v0, [1, 2, 3, 8, 9, 10], HY, HY + ROWS)
        sweep(v0, v1, outer, HY + 1, HY + ROWS - 1)

    def presmooth_window():
        window_inside()
        arrived(forwarded)
        sent(later)
        for lo, hi in ((0, HY), (HY + ROWS, NYW)):
            start_from_zero(v0, inner, lo, hi)
        sweep(v0, v1, own_layers, 1, HY - 1)
        sweep(v0, v1, own_layers, HY + ROWS + 1, NYW - 1)
        sweep(v0, v1, outer, 1, HY + 1)
        sweep(v0, v1, outer, HY + ROWS - 1, NYW - 1)

    coarse_cycle(0, background_one, forward_last, presmooth_window)
    arrived(later)
    correct(all_layers, H1 - 1, H1 + 5, (1, NYW - 2), lambda w, y: v1[w, rows_of(y), :], v1)
    bufs = (v1, v0)
    for s in range(4):
        sweep(bufs[s % 2], bufs[(s + 1) % 2], list(range(s + 1, NW - 1 - s)), s + 2, NYW - 2 - s)
    restricted_residual(v1, 1)

    tail = []

    def background_two():
        tail.extend([
            push(v1.at[pl.ds(5, 3), own], v2.at[pl.ds(1, 3), own], 1, 0),
            push(v1.at[pl.ds(4, 3), own], v2.at[pl.ds(8, 3), own], -1, 0),
            push(v1.at[pl.ds(4, 4), rows_of(last - 2, 3)], v2.at[pl.ds(4, 4), rows_of(HY - 3, 3)], 0, 1),
            push(v1.at[pl.ds(4, 4), rows_of(HY, 3)], v2.at[pl.ds(4, 4), rows_of(last + 1, 3)], 0, -1),
            push(v1.at[pl.ds(6, 2), rows_of(last - 1, 2)], v2.at[pl.ds(2, 2), rows_of(HY - 2, 2)], 1, 1),
            push(v1.at[pl.ds(6, 2), rows_of(HY, 2)], v2.at[pl.ds(2, 2), rows_of(last + 1, 2)], 1, -1),
            push(v1.at[pl.ds(4, 2), rows_of(last - 1, 2)], v2.at[pl.ds(8, 2), rows_of(HY - 2, 2)], -1, 1),
            push(v1.at[pl.ds(4, 2), rows_of(HY, 2)], v2.at[pl.ds(8, 2), rows_of(last + 1, 2)], -1, -1),
        ])

    coarse_cycle(1, background_two, lambda: None, lambda: None)
    arrived(tail)

    def keep_own(y):
        for w in own_layers:
            v2[w, rows_of(y), :] = v1[w, rows_of(y), :]

    row_loop(HY, HY + ROWS, 4, keep_own)
    deep = list(range(1, NW - 1))
    correct(deep, H1 - 1, H1 + 5, (), lambda w, y: v2[w, rows_of(y), :], v0)
    sent(tail)
    sweep(v0, v1, deep[1:-1], HY - 2, HY + ROWS + 2)
    sweep(v1, v0, deep[2:-2], HY - 1, HY + ROWS + 1)

    def defect(y, count):
        for w in own_layers:
            for j, (x, total) in enumerate(flows(v0, w, y, count)):
                v2[w, rows_of(y + j), :] = total - diagonal(w, y + j) * x

    strip_loop(HY, HY + ROWS, 4, defect)

    for k in range(K):
        block = jnp.concatenate([src[w, pl.ds(HY * K + k, ROWS, stride=K), :]
                                 for src in (v0, v2) for w in own_layers], axis=0)
        out[pl.ds(k, LANES, stride=K), :] = block.T
    sent(par + near + bulk + far_source + forwarded)


OUT_PARTS = 4


def natural(turned_in, v_out, b_out, turned, v_vm, b_vm, sem):
    copies = []
    per = K // OUT_PARTS
    loads = []
    for g in range(OUT_PARTS):
        part = pl.ds(g * per * LANES, per * LANES)
        loads.append(pltpu.make_async_copy(turned_in.at[part], turned.at[part], sem.at[2, g]))
        loads[g].start()
    for g in range(OUT_PARTS):
        loads[g].wait()
        for m in range(g * per, (g + 1) * per):
            block = turned[m * LANES:(m + 1) * LANES, :].T
            v_vm[:, :, m * LANES:(m + 1) * LANES] = block[0:LZ * ROWS].reshape(LZ, ROWS, LANES)
            b_vm[:, :, m * LANES:(m + 1) * LANES] = block[LZ * ROWS:].reshape(LZ, ROWS, LANES)
        part = (slice(None), slice(None), pl.ds(g * per * LANES, per * LANES))
        for i, (src, dst) in enumerate(((v_vm, v_out), (b_vm, b_out))):
            copies.append(pltpu.make_async_copy(src.at[part], dst.at[part], sem.at[i, g]))
            copies[-1].start()
    for copy in copies:
        copy.wait()


N_COPIES = 3 + 8 + 4 + 8 + 12 + 8 + 2 * (3 + 6 + 2 * H2)


def local(n_tile, source_heating, material_thermal_values, layer_material, via_conductance, via_blocks):
    def tiles(*lead):
        return pltpu.VMEM(lead + (NZ, LANES), F32)

    def window(n):
        return pltpu.VMEM((n, NYW * K, LANES), F32)

    vmem = pl.BlockSpec(memory_space=pltpu.VMEM)
    shape = jax.ShapeDtypeStruct(source_heating.shape, F32)
    turned = pl.pallas_call(
        functools.partial(kernel, n_tile),
        out_shape=jax.ShapeDtypeStruct((K * LANES, LANES), F32),
        in_specs=[pl.BlockSpec(memory_space=pltpu.HBM)] * 5,
        out_specs=vmem,
        scratch_shapes=[
            pltpu.SMEM(material_thermal_values.shape, F32), pltpu.SMEM(layer_material.shape, jnp.int32),
            pltpu.SMEM(via_conductance.shape, F32), pltpu.VMEM((1, 4, via_blocks.shape[1]), jnp.int32),
            pltpu.VMEM(source_heating.shape, F32),
            window(NW), window(NW), window(NW), window(NW), window(4),
            pltpu.VMEM((NYW * K, LANES), F32), window(3), window(3),
            pltpu.VMEM((4, 8, LANES), F32), tiles(2),
            pltpu.VMEM((K * LANES, LANES), F32), pltpu.VMEM((4 * 6 * K, LANES), F32),
            pltpu.VMEM((2, 4, 12, 8, LANES), F32), tiles(2, N1 * 4),
            tiles(N1 * 4), tiles(N1 * 4), tiles(N1 * 4), tiles(N1 * 4), tiles(N1 * 4),
            tiles(2, N2), tiles(N2), tiles(N2), tiles(N2), tiles(N2), tiles(N2),
            pltpu.VMEM((4, 80, LANES), F32), pltpu.VMEM((8, LANES), F32),
            pltpu.VMEM((NW, 8, LANES), F32),
            pltpu.SemaphoreType.DMA((N_COPIES,)),
            pltpu.SemaphoreType.DMA((N_COPIES,)),
            pltpu.SemaphoreType.DMA((8,)),
        ],
        compiler_params=pltpu.CompilerParams(collective_id=0, has_side_effects=True),
    )(source_heating, material_thermal_values, layer_material, via_conductance, via_blocks.transpose(0, 2, 1))
    anywhere = pl.BlockSpec(memory_space=pl.ANY)
    return pl.pallas_call(
        natural,
        out_shape=(shape, shape),
        in_specs=[anywhere],
        out_specs=(anywhere, anywhere),
        scratch_shapes=[pltpu.VMEM((K * LANES, LANES), F32), pltpu.VMEM(source_heating.shape, F32), pltpu.VMEM(source_heating.shape, F32),
                        pltpu.SemaphoreType.DMA((3, OUT_PARTS))],
    )(turned)


def solution(mesh):
    in_specs = (P("die", "tile", None), P(), P("die"), P("die"), P("die", None, None))
    out_specs = (P("die", "tile", None), P("die", "tile", None))
    body = functools.partial(local, mesh.shape["tile"])
    return jax.shard_map(body, mesh=mesh, in_specs=in_specs, out_specs=out_specs, check_vma=False)
```
